32 devices in a mesh: row: 4 (over y, core), col: 8 (over z, x).
Axes of the slice: x: 2, y: 2, z: 4, core: 2. Of those that a mesh axis runs over, the one named last changes fastest.
Arguments:
- velocity_modes: bfloat16 [3, 176, 352, 704], P(None, 'row', 'col'), may hold values from -0.00090789795 to 0.00090789795
- wavenumbers: float32 [8], replicated, may hold values from 0.5 to 3
- polar: float32 [8], replicated, may hold values from -3.140625 to 3.140625
- azimuth: float32 [8], replicated, may hold values from -3.140625 to 3.140625
Outputs:
- velocity: bfloat16 [3, 512, 512, 512], P(None, 'row', 'col')
- far_field: float32 [8, 2, 8], P('col')
The draws below stay inside these ranges and needn't reach their ends.
All inputs are finite; a program needn't handle non-finite values.
Results may differ from the reference program's by a relative error of at most 0.0075.
Values may be sent and summed in bfloat16 or wider, within the bound.
A program may use at most 192 MiB of HBM per device.

```python
import math
import jax
import jax.numpy as jnp
from jax import lax

N = 512
M = 352
KX = 176
FREQS = 8
DIRS = 8


def levels(rng, extent, split, low, largest):
    factor_of, own = 1.0, jax.random.fold_in(rng, 6)
    for axis_at, blocks in split:
        draws = jnp.exp(jax.random.uniform(jax.random.fold_in(own, axis_at), (blocks,), jnp.float32, low / len(split), largest / len(split)))
        factor_of = factor_of * jnp.repeat(draws, extent[axis_at] // blocks).reshape([-1 if axis == axis_at else 1 for axis in range(len(extent))])
    return factor_of


def scatter_about(key, shape, width, most, cuts=(), kind=jnp.bfloat16):
    factor_of = levels(key, shape, cuts, -0.22, 0.18) if cuts else 1.0
    drawn = jax.random.normal(key, shape, jnp.float32) * width * factor_of
    return jnp.minimum(jnp.maximum(drawn, -most), most).astype(kind)


def setup_inputs(seed: int = 0) -> dict:
    streams_of = jax.random.split(jax.random.key(seed), 5)
    return {
        "velocity_modes": scatter_about(streams_of[0], (3, KX, M, 2 * M), (M ** -1.5), 0.00090789795, ((1, 4), (2, 8))),
        "wavenumbers": jnp.clip(jnp.exp(jax.random.uniform(streams_of[1], (FREQS,), jnp.float32, math.log(0.5), math.log(3.0))), 0.5, 3.0),
        "polar": jnp.clip(jax.random.uniform(streams_of[2], (DIRS,), jnp.float32, -3.140625, 3.140625), -3.140625, 3.140625),
        "azimuth": jnp.clip(jax.random.uniform(streams_of[3], (DIRS,), jnp.float32, -3.140625, 3.140625), -3.140625, 3.140625),
    }


def complex_table(modes, points):
    waves = jnp.arange(modes, dtype=jnp.int32) - modes // 2
    cells = jnp.arange(points, dtype=jnp.int32)
    product = jnp.mod(waves[:, None] * cells[None, :], points)
    angle = product.astype(jnp.float32) * (2.0 * math.pi / points)
    cosine = jnp.cos(angle)
    sine = jnp.sin(angle)
    table = jnp.stack([jnp.stack([cosine, sine], 1), jnp.stack([-sine, cosine], 1)], 0)
    return table.astype(jnp.bfloat16)


def half_table(count, points):
    waves = jnp.arange(count, dtype=jnp.int32)
    cells = jnp.arange(points, dtype=jnp.int32)
    product = jnp.mod(waves[:, None] * cells[None, :], points)
    angle = product.astype(jnp.float32) * (2.0 * math.pi / points)
    cosine = jnp.cos(angle).astype(jnp.bfloat16)
    sine = jnp.sin(angle).astype(jnp.bfloat16)
    factor = jnp.where(waves == 0, 1.0, 2.0).astype(jnp.bfloat16)[:, None]
    return jnp.stack([factor * cosine, -(factor * sine)], 0)


def stresses(field):
    trace = (field[0] * field[0] + field[1] * field[1] + field[2] * field[2]) / 3.0
    parts = [field[0] * field[0] - trace, field[1] * field[1] - trace, field[2] * field[2] - trace,
             field[0] * field[1], field[0] * field[2], field[1] * field[2]]
    return jnp.stack(parts, 0).astype(jnp.bfloat16)


def far_terms(stress, wave_j, axis_one, axis_two, axis_three, y_pos, z_pos):
    points = stress.shape[-1]
    y_count = stress.shape[1]
    z_count = stress.shape[2]
    count = wave_j.shape[0]
    x_pos = jnp.arange(points, dtype=jnp.int32).astype(jnp.float32) * (2.0 * math.pi / points)
    angle_x = wave_j[None, :] * (axis_one[None, :] * x_pos[:, None])
    phase_x = jnp.stack([jnp.cos(angle_x), -jnp.sin(angle_x)], 1).reshape(points, 2 * count).astype(jnp.bfloat16)
    lines = jnp.dot(stress.reshape(6 * y_count * z_count, points), phase_x, preferred_element_type=jnp.float32)
    lines = lines.reshape(6, y_count, z_count, 2, count)
    weights = [axis_one * axis_one, axis_two * axis_two, axis_three * axis_three,
               2.0 * axis_one * axis_two, 2.0 * axis_one * axis_three, 2.0 * axis_two * axis_three]
    mixed = weights[0][None, None, None, :] * lines[0]
    for index in range(1, 6):
        mixed = mixed + weights[index][None, None, None, :] * lines[index]
    angle = wave_j[None, None, :] * (axis_two[None, None, :] * y_pos[:, None, None]) + wave_j[None, None, :] * (axis_three[None, None, :] * z_pos[None, :, None])
    cosine = jnp.cos(angle)
    sine = jnp.sin(angle)
    real_part = mixed[:, :, 0, :]
    imag_part = mixed[:, :, 1, :]
    return jnp.stack([jnp.sum(real_part * cosine + imag_part * sine, (0, 1)),
                      jnp.sum(imag_part * cosine - real_part * sine, (0, 1))], 0)


def reference(velocity_modes, wavenumbers, polar, azimuth):
    table = complex_table(M, N)
    table_x = half_table(KX, N)
    modes = velocity_modes.reshape(3, KX, M, 2, M)

    def along_z(component):
        return jnp.einsum("abpk,pkqz->azqb", component.astype(jnp.float32), table.astype(jnp.float32)).astype(jnp.bfloat16)

    first = lax.map(along_z, modes)

    def along_y(component):
        return jnp.einsum("azpb,pbqy->yzqa", component.astype(jnp.float32), table.astype(jnp.float32)).astype(jnp.bfloat16)

    second = lax.map(along_y, first)
    dirs = polar.shape[0]
    wave_j = jnp.repeat(wavenumbers, dirs)
    axis_one = jnp.tile(jnp.sin(polar) * jnp.cos(azimuth), FREQS)
    axis_two = jnp.tile(jnp.sin(polar) * jnp.sin(azimuth), FREQS)
    axis_three = jnp.tile(jnp.cos(polar), FREQS)
    block = 8
    z_pos = jnp.arange(N, dtype=jnp.int32).astype(jnp.float32) * (2.0 * math.pi / N)

    def one_block(number):
        start = (number * block).astype(jnp.int32)
        piece = lax.dynamic_slice_in_dim(second, start, block, 1)
        field = jnp.einsum("cyzpa,pax->cyzx", piece.astype(jnp.float32), table_x.astype(jnp.float32))
        stress = stresses(field)
        y_pos = (start + jnp.arange(block, dtype=jnp.int32)).astype(jnp.float32) * (2.0 * math.pi / N)
        terms = far_terms(stress, wave_j, axis_one, axis_two, axis_three, y_pos, z_pos)
        return field.astype(jnp.bfloat16), terms

    blocks, terms = lax.map(one_block, jnp.arange(N // block, dtype=jnp.int32))
    velocity = jnp.transpose(blocks, (1, 0, 2, 3, 4)).reshape(3, N, N, N)
    spectrum = jnp.sum(terms, 0).reshape(2, FREQS, dirs)
    spectrum = spectrum * (wavenumbers * wavenumbers)[None, :, None] / (N ** 1.5)
    far_field = jnp.transpose(spectrum, (2, 0, 1))
    return velocity, far_field
```

```python
import functools
import math

import jax
import jax.numpy as jnp
from jax import lax
from jax.experimental import pallas as pl
from jax.experimental.pallas import tpu as pltpu
from jax.sharding import PartitionSpec as P

VMEM_LIMIT = 60 * 1024 * 1024


def padded(count):
    return -(-count // 16) * 16


def phases(waves, cells, points):
    product = jnp.mod(waves[:, None] * cells[None, :], points)
    return product.astype(jnp.float32) * (2.0 * math.pi / points)


def turned(count, axis, step):
    return jnp.mod(lax.axis_index(axis) + step * jnp.arange(count, dtype=jnp.int32), count)


def z_table(modes, points, blocks):
    cells = points // blocks
    owner = turned(blocks, "col", 1)
    at = (owner[:, None] * cells + jnp.arange(cells, dtype=jnp.int32)[None, :]).reshape(-1)
    waves = jnp.arange(modes, dtype=jnp.int32) - modes // 2
    angle = phases(waves, at, points)
    cosine = jnp.cos(angle).reshape(modes, blocks, 1, -1)
    sine = jnp.sin(angle).reshape(modes, blocks, 1, -1)
    table = jnp.concatenate(
        [jnp.concatenate([cosine, sine], 2), jnp.concatenate([-sine, cosine], 2)], 0
    )
    return table.reshape(2 * modes, 2 * points).astype(jnp.bfloat16)


def y_table(modes, points, sources, blocks):
    cells, held = points // blocks, modes // sources
    extra = padded(held)
    owner = turned(blocks, "row", 1)
    at = owner[:, None] * cells + jnp.arange(cells, dtype=jnp.int32)[None, :]
    slot = jnp.arange(extra, dtype=jnp.int32)
    waves = turned(sources, "col", -1)[:, None] * held + slot[None, :] - modes // 2
    angle = phases(at.reshape(-1), waves.reshape(-1), points)
    keep = jnp.tile(slot < held, sources)[None, :]
    both = jnp.stack([jnp.where(keep, jnp.cos(angle), 0.0), jnp.where(keep, jnp.sin(angle), 0.0)], 0)
    both = both.reshape(2, blocks, cells, -1)
    return jnp.transpose(both, (1, 0, 2, 3)).reshape(blocks, 2 * cells, -1).astype(jnp.bfloat16)


def x_table(count, points, sources):
    held = count // sources
    extra = padded(held)
    slot = jnp.arange(extra, dtype=jnp.int32)
    waves = (turned(sources, "row", -1)[:, None] * held + slot[None, :]).reshape(-1)
    keep = jnp.tile(slot < held, sources)
    angle = phases(waves, jnp.arange(points, dtype=jnp.int32), points)
    cosine = jnp.cos(angle).astype(jnp.bfloat16)
    sine = jnp.sin(angle).astype(jnp.bfloat16)
    factor = jnp.where(keep, jnp.where(waves == 0, 1.0, 2.0), 0.0).astype(jnp.bfloat16)[:, None]
    return jnp.stack([factor * cosine, -(factor * sine)], 0)


def estimate(rows, depth, columns):
    return pl.CostEstimate(
        flops=2 * rows * depth * columns,
        bytes_accessed=2 * (rows * depth + depth * columns + rows * columns),
        transcendentals=0,
    )


MESH = pl.DeviceIdType.MESH
CHUNK = 16


def exchange(rows, cols, modes_ref, table_z, table_y, out_ref, modes, sent, came, total, passed,
             in_sem, send_z, recv_z, send_y, recv_y):
    kx, ky = modes.shape[1], modes.shape[2]
    ky_pad, width = came.shape[3], came.shape[4]
    half = width // 2
    y_local = out_ref.shape[2]
    at_col, at_row = lax.axis_index("col"), lax.axis_index("row")
    pieces = [(start, min(CHUNK, kx - start)) for start in range(0, kx, CHUNK)]
    count = len(pieces)
    col_peer = [lax.rem(at_col + r, cols) for r in range(cols)]
    row_peer = [lax.rem(at_row + r, rows) for r in range(rows)]

    def load(c):
        return pltpu.make_async_copy(modes_ref.at[c], modes.at[c], in_sem.at[c])

    for c in range(3):
        load(c).start()
    barrier = pltpu.get_barrier_semaphore()
    for r in range(1, cols):
        pl.semaphore_signal(barrier, inc=1, device_id={"col": col_peer[r]}, device_id_type=MESH)
    for r in range(1, rows):
        pl.semaphore_signal(barrier, inc=1, device_id={"row": row_peer[r]}, device_id_type=MESH)

    def z_copy(t, r, size):
        return pltpu.make_async_remote_copy(
            src_ref=sent.at[t, r - 1, pl.ds(0, size)], dst_ref=came.at[t, r, pl.ds(0, size)],
            send_sem=send_z.at[t, r], recv_sem=recv_z.at[t, r],
            device_id={"col": col_peer[r]}, device_id_type=MESH)

    def y_copy(c, j, r):
        return pltpu.make_async_remote_copy(
            src_ref=passed.at[j, r], dst_ref=out_ref.at[r, c, :, pl.ds(j * CHUNK, CHUNK), :],
            send_sem=send_y.at[c, j, r], recv_sem=recv_y.at[c, j, r],
            device_id={"row": row_peer[r]}, device_id_type=MESH)

    def y_own(c, j):
        return pltpu.make_async_copy(
            passed.at[j, 0], out_ref.at[0, c, :, pl.ds(j * CHUNK, CHUNK), :], send_y.at[c, j, 0])

    total[...] = jnp.zeros_like(total)

    @pl.loop(0, 3)
    def _(c):
        load(c).wait()
        for j, (start, size) in enumerate(pieces):
            t = c * count + j

            @pl.loop(0, size)
            def _(a):
                value = jnp.dot(modes[c, start + a], table_z[...], preferred_element_type=jnp.float32)
                value = value.astype(jnp.bfloat16)
                for r in range(cols):
                    to = came.at[t, 0, a] if r == 0 else sent.at[t, r - 1, a]
                    to[...] = jnp.zeros(to.shape, jnp.bfloat16)
                    to[0:ky, :] = value[:, r * width : (r + 1) * width]

            if j == 0:
                @pl.when(c == 0)
                def _():
                    pl.semaphore_wait(barrier, cols + rows - 2)
            for r in range(1, cols):
                z_copy(t, r, size).start()

    @pl.loop(0, 3)
    def _(c):
        for j, (start, size) in enumerate(pieces):
            t = c * count + j
            for r in range(1, cols):
                z_copy(t, r, size).wait_recv()

            @pl.when(c > 0)
            def _():
                y_own(c - 1, j).wait()
                for r in range(1, rows):
                    y_copy(c - 1, j, r).wait_send()

            group = 2 if size % 2 == 0 and width % 128 == 0 else 1

            @pl.loop(0, rows)
            def _(b):
                for a in range(0, size, group):
                    parts = [came[t, :, a + g].reshape(-1, width) for g in range(group)]
                    data = parts[0] if group == 1 else jnp.concatenate(parts, 1)
                    product = jnp.dot(table_y[b], data, preferred_element_type=jnp.float32)
                    for g in range(group):
                        by_cos = product[:y_local, g * width : (g + 1) * width]
                        by_sin = product[y_local:, g * width : (g + 1) * width]
                        swap = jnp.concatenate([-by_sin[:, half:], by_sin[:, :half]], 1)
                        total[:, a + g, :] = by_cos + swap
                if size < CHUNK:
                    total[:, size:, :] = jnp.zeros((y_local, CHUNK - size, width), jnp.float32)
                passed[j, b] = total[...].astype(jnp.bfloat16)

            y_own(c, j).start()
            for r in range(1, rows):
                y_copy(c, j, r).start()

    @pl.loop(0, 3)
    def _(c):
        for j, (start, size) in enumerate(pieces):
            for r in range(1, cols):
                z_copy(c * count + j, r, size).wait_send()
            for r in range(1, rows):
                y_copy(c, j, r).wait_recv()

    for j in range(count):
        y_own(2, j).wait()
        for r in range(1, rows):
            y_copy(2, j, r).wait_send()


def along_x(arrived_0, arrived_1, arrived_2, table_ref, phase_ref, weight_ref, cos_ref, sin_ref,
            velocity_ref, by_cos_ref, by_sin_ref, real_scr, imag_scr):
    ys, width = arrived_0.shape[2], arrived_0.shape[4]
    half = width // 2
    fields = []
    for c, arrived_ref in enumerate((arrived_0, arrived_1, arrived_2)):
        for y in range(ys):
            data = arrived_ref[:, 0, y].reshape(-1, width).T
            real_scr[c, y * half : (y + 1) * half, :] = data[:half]
            imag_scr[c, y * half : (y + 1) * half, :] = data[half:]
        field = jnp.dot(real_scr[c], table_ref[0], preferred_element_type=jnp.float32)
        field = field + jnp.dot(imag_scr[c], table_ref[1], preferred_element_type=jnp.float32)
        velocity_ref[c] = field.astype(jnp.bfloat16).reshape(velocity_ref.shape[1:])
        fields.append(field)
    f0, f1, f2 = fields
    trace = (f0 * f0 + f1 * f1 + f2 * f2) / 3.0
    stress = [f0 * f0 - trace, f1 * f1 - trace, f2 * f2 - trace, f0 * f1, f0 * f2, f1 * f2]
    mixed = None
    for index, part in enumerate(stress):
        line = jnp.dot(
            part.astype(jnp.bfloat16), phase_ref[...], preferred_element_type=jnp.float32
        )
        term = weight_ref[index : index + 1, :] * line
        mixed = term if mixed is None else mixed + term
    mixed = mixed.reshape(ys, half, -1)
    by_cos_ref[...] = jnp.sum(mixed * cos_ref[...][None], 1)
    by_sin_ref[...] = jnp.sum(mixed * sin_ref[...][None], 1)


def body(rows, cols, velocity_modes, wavenumbers, polar, azimuth):
    kx_local, ky_local, modes = velocity_modes.shape[1:]
    modes = modes // 2
    kx = kx_local * rows
    points = velocity_points(modes)
    y_local, z_local = points // rows, points // cols
    width = 2 * z_local
    ky_pad, kx_pad = padded(ky_local), padded(kx_local)

    table_z = z_table(modes, points, cols)
    table_y = y_table(modes, points, cols, rows)
    count_t = 3 * (kx_pad // CHUNK)
    arrived = pl.pallas_call(
        functools.partial(exchange, rows, cols),
        in_specs=[
            pl.BlockSpec(memory_space=pl.ANY),
            pl.BlockSpec(memory_space=pltpu.VMEM),
            pl.BlockSpec(memory_space=pltpu.VMEM),
        ],
        out_specs=pl.BlockSpec(memory_space=pl.ANY),
        out_shape=jax.ShapeDtypeStruct((rows, 3, y_local, kx_pad, width), jnp.bfloat16),
        scratch_shapes=[
            pltpu.VMEM(velocity_modes.shape, jnp.bfloat16),
            pltpu.VMEM((count_t, cols - 1, CHUNK, ky_pad, width), jnp.bfloat16),
            pltpu.VMEM((count_t, cols, CHUNK, ky_pad, width), jnp.bfloat16),
            pltpu.VMEM((y_local, CHUNK, width), jnp.float32),
            pltpu.VMEM((kx_pad // CHUNK, rows, y_local, CHUNK, width), jnp.bfloat16),
            pltpu.SemaphoreType.DMA((3,)),
            pltpu.SemaphoreType.DMA((count_t, cols)),
            pltpu.SemaphoreType.DMA((count_t, cols)),
            pltpu.SemaphoreType.DMA((3, kx_pad // CHUNK, rows)),
            pltpu.SemaphoreType.DMA((3, kx_pad // CHUNK, rows)),
        ],
        compiler_params=pltpu.CompilerParams(
            vmem_limit_bytes=VMEM_LIMIT, collective_id=0, has_side_effects=True
        ),
        cost_estimate=estimate(3 * 2 * points, cols * ky_pad, 2 * kx_local * width),
        name="exchange",
    )(velocity_modes, table_z, table_y)

    dirs, freqs = polar.shape[0], wavenumbers.shape[0]
    count = dirs * freqs
    wave_j = jnp.repeat(wavenumbers, dirs)
    axis_one = jnp.tile(jnp.sin(polar) * jnp.cos(azimuth), freqs)
    axis_two = jnp.tile(jnp.sin(polar) * jnp.sin(azimuth), freqs)
    axis_three = jnp.tile(jnp.cos(polar), freqs)
    unit = 2.0 * math.pi / points
    x_pos = jnp.arange(points, dtype=jnp.int32).astype(jnp.float32) * unit
    angle_x = wave_j[None, :] * (axis_one[None, :] * x_pos[:, None])
    phase_x = jnp.concatenate([jnp.cos(angle_x), -jnp.sin(angle_x)], 1).astype(jnp.bfloat16)
    weights = jnp.stack(
        [
            axis_one * axis_one,
            axis_two * axis_two,
            axis_three * axis_three,
            2.0 * axis_one * axis_two,
            2.0 * axis_one * axis_three,
            2.0 * axis_two * axis_three,
        ],
        0,
    )
    weights = jnp.concatenate([weights, weights], 1)
    z_index = lax.axis_index("col") * z_local + jnp.arange(z_local, dtype=jnp.int32)
    y_index = lax.axis_index("row") * y_local + jnp.arange(y_local, dtype=jnp.int32)
    angle_z = wave_j[None, :] * (axis_three[None, :] * (z_index.astype(jnp.float32) * unit)[:, None])
    angle_y = wave_j[None, :] * (axis_two[None, :] * (y_index.astype(jnp.float32) * unit)[:, None])
    cos_z, sin_z = jnp.cos(angle_z), jnp.sin(angle_z)

    ys = 8
    whole = lambda i: (0, 0)
    velocity, by_cos, by_sin = pl.pallas_call(
        along_x,
        grid=(y_local // ys,),
        in_specs=[
            *[
                pl.BlockSpec((rows, 1, ys, kx_pad, width), lambda i, c=c: (0, c, i, 0, 0))
                for c in range(3)
            ],
            pl.BlockSpec((2, rows * kx_pad, points), lambda i: (0, 0, 0)),
            pl.BlockSpec((points, 2 * count), whole),
            pl.BlockSpec((6, 2 * count), whole),
            pl.BlockSpec((z_local, 2 * count), whole),
            pl.BlockSpec((z_local, 2 * count), whole),
        ],
        out_specs=[
            pl.BlockSpec((3, ys, z_local, points), lambda i: (0, i, 0, 0)),
            pl.BlockSpec((ys, 2 * count), lambda i: (i, 0)),
            pl.BlockSpec((ys, 2 * count), lambda i: (i, 0)),
        ],
        out_shape=[
            jax.ShapeDtypeStruct((3, y_local, z_local, points), jnp.bfloat16),
            jax.ShapeDtypeStruct((y_local, 2 * count), jnp.float32),
            jax.ShapeDtypeStruct((y_local, 2 * count), jnp.float32),
        ],
        scratch_shapes=[pltpu.VMEM((3, ys * z_local, rows * kx_pad), jnp.bfloat16)] * 2,
        compiler_params=pltpu.CompilerParams(vmem_limit_bytes=VMEM_LIMIT),
        name="along_x",
    )(
        arrived,
        arrived,
        arrived,
        x_table(kx, points, rows),
        phase_x,
        weights,
        jnp.concatenate([cos_z, cos_z], 1),
        jnp.concatenate([sin_z, sin_z], 1),
    )
    real_part = by_cos[:, :count] + by_sin[:, count:]
    imag_part = by_cos[:, count:] - by_sin[:, :count]
    cos_y, sin_y = jnp.cos(angle_y), jnp.sin(angle_y)
    terms = jnp.stack(
        [
            jnp.sum(real_part * cos_y + imag_part * sin_y, 0),
            jnp.sum(imag_part * cos_y - real_part * sin_y, 0),
        ],
        0,
    )
    spectrum = terms.reshape(2, freqs, dirs) * (wavenumbers * wavenumbers)[None, :, None]
    spectrum = jnp.transpose(spectrum / points**1.5, (2, 0, 1))
    total = lax.psum(spectrum, ("row", "col"))
    owned = dirs // cols
    far_field = lax.dynamic_slice_in_dim(total, lax.axis_index("col") * owned, owned, 0)
    return (velocity, far_field)


def velocity_points(modes):
    return 1 << (modes - 1).bit_length()


def solution(mesh):
    return jax.shard_map(
        functools.partial(body, mesh.shape["row"], mesh.shape["col"]),
        mesh=mesh,
        in_specs=(P(None, "row", "col", None), P(), P(), P()),
        out_specs=(P(None, "row", "col", None), P("col", None, None)),
        check_vma=False,
    )
```

```python
import functools
import math

import jax
import jax.numpy as jnp
import numpy as np
from jax import lax
from jax.experimental import pallas as pl
from jax.experimental.pallas import tpu as pltpu
from jax.sharding import PartitionSpec as P

VMEM_LIMIT = 60 * 1024 * 1024


def padded(count):
    return -(-count // 16) * 16


def circle(waves, cells, points):
    angle = np.mod(np.outer(waves, cells), points).astype(np.float64) * (2.0 * math.pi / points)
    return np.cos(angle).astype(np.float32), np.sin(angle).astype(np.float32)


def z_table(modes, points, blocks):
    cosine, sine = circle(np.arange(modes) - modes // 2, np.arange(points), points)
    cosine, sine = (part.reshape(modes, blocks, 1, -1) for part in (cosine, sine))
    table = np.concatenate(
        [np.concatenate([cosine, sine], 2), np.concatenate([-sine, cosine], 2)], 0
    )
    return jnp.asarray(table.reshape(2 * modes, 2 * points).astype(jnp.bfloat16))


def y_table(modes, points, sources, blocks, held_rows):
    cosine, sine = circle(np.arange(points), np.arange(modes) - modes // 2, points)
    both = np.stack([cosine, sine], 0)
    both = both.reshape(2, blocks, points // blocks, sources, modes // sources)
    extra = held_rows - modes // sources
    both = np.pad(both, ((0, 0), (0, 0), (0, 0), (0, 0), (0, extra)))
    both = np.transpose(both, (1, 0, 2, 3, 4))
    return jnp.asarray(both.reshape(blocks, 2 * (points // blocks), -1).astype(jnp.bfloat16))


def x_table(count, points, sources):
    cosine, sine = circle(np.arange(count), np.arange(points), points)
    factor = np.where(np.arange(count) == 0, 1.0, 2.0).astype(np.float32)[:, None]
    cosine, sine = (part.astype(jnp.bfloat16).astype(np.float32) for part in (cosine, sine))
    table = np.stack([factor * cosine, -(factor * sine)], 0)
    table = table.reshape(2, sources, count // sources, points)
    extra = padded(count // sources) - count // sources
    table = np.pad(table, ((0, 0), (0, 0), (0, extra), (0, 0)))
    return jnp.asarray(table.reshape(2, -1, points).astype(jnp.bfloat16))


def estimate(rows, depth, columns):
    return pl.CostEstimate(
        flops=2 * rows * depth * columns,
        bytes_accessed=2 * (rows * depth + depth * columns + rows * columns),
        transcendentals=0,
    )


MESH = pl.DeviceIdType.MESH
CHUNK = 8
SLOTS = 3


def grouping(kx, ky):
    if kx % 4 == 0 and ky % 4 == 0:
        return 4, ky
    return 1, padded(ky)


def pieces_of(kx):
    return [(start, min(CHUNK, kx - start)) for start in range(0, kx, CHUNK)]


def exchange(rows, cols, modes_ref, table_z, table_y, out_ref, modes, sent, came, ready, total, passed,
             in_sem, send_z, recv_z, send_y, recv_y):
    kx, ky = modes.shape[1], modes.shape[2]
    width = came.shape[3]
    half = width // 2
    y_local = out_ref.shape[2]
    at_col, at_row = lax.axis_index("col"), lax.axis_index("row")
    group, held = grouping(kx, ky)
    block = group * held
    pieces = pieces_of(kx)
    count = len(pieces)
    pair = ready.shape[2] // width

    def load(c):
        return pltpu.make_async_copy(modes_ref.at[c], modes.at[c], in_sem.at[c])

    for c in range(3):
        load(c).start()
    barrier = pltpu.get_barrier_semaphore()
    for r in range(1, cols):
        peer = lax.rem(at_col + r, cols)
        pl.semaphore_signal(barrier, inc=1, device_id={"col": peer}, device_id_type=MESH)
    for r in range(1, rows):
        peer = lax.rem(at_row + r, rows)
        pl.semaphore_signal(barrier, inc=1, device_id={"row": peer}, device_id_type=MESH)

    def z_copy(t, r, size):
        peer = lax.rem(at_col + r, cols)
        used = pl.ds(0, size * held)
        return pltpu.make_async_remote_copy(
            src_ref=sent.at[t, peer, used], dst_ref=came.at[t, at_col, used],
            send_sem=send_z.at[t, r], recv_sem=recv_z.at[t, r],
            device_id={"col": peer}, device_id_type=MESH)

    def y_copy(c, j, r):
        peer = lax.rem(at_row + r, rows)
        return pltpu.make_async_remote_copy(
            src_ref=passed.at[j % SLOTS, peer],
            dst_ref=out_ref.at[at_row, c, :, pl.ds(j * CHUNK, CHUNK), :],
            send_sem=send_y.at[c, j, r], recv_sem=recv_y.at[c, j, r],
            device_id={"row": peer}, device_id_type=MESH)

    def y_own(c, j):
        return pltpu.make_async_copy(
            passed.at[j % SLOTS, at_row],
            out_ref.at[at_row, c, :, pl.ds(j * CHUNK, CHUNK), :], send_y.at[c, j, 0])

    def y_left(c, j):
        y_own(c, j).wait()
        for r in range(1, rows):
            y_copy(c, j, r).wait_send()

    total[...] = jnp.zeros_like(total)

    @pl.loop(0, 3)
    def _(c):
        load(c).wait()
        for j, (start, size) in enumerate(pieces):
            t = c * count + j

            @pl.loop(0, size // group)
            def _(g):
                slabs = [modes[c, start + g * group + i] for i in range(group)]
                data = slabs[0] if group == 1 else jnp.concatenate(slabs, 0)
                value = jnp.dot(data, table_z[...], preferred_element_type=jnp.float32)
                value = value.astype(jnp.bfloat16)
                if value.shape[0] < block:
                    spare = jnp.zeros((block - value.shape[0], value.shape[1]), jnp.bfloat16)
                    value = jnp.concatenate([value, spare], 0)
                at = pl.ds(pl.multiple_of(g * block, 16), block)
                for b in range(cols):
                    sent[t, b, at, :] = value[:, b * width : (b + 1) * width]
                came[t, at_col, at, :] = sent[t, at_col, at, :]

            if j == 0:
                @pl.when(c == 0)
                def _():
                    pl.semaphore_wait(barrier, cols + rows - 2)
            for r in range(1, cols):
                z_copy(t, r, size).start()

    @pl.loop(0, 3)
    def _(c):
        for j, (start, size) in enumerate(pieces):
            t = c * count + j
            for r in range(1, cols):
                z_copy(t, r, size).wait_recv()

            @pl.loop(0, size // group)
            def _(g):
                at = pl.ds(pl.multiple_of(g * block, 16), block)
                blocks = [came[t, s, at, :] for s in range(cols)]
                lines = []
                for i in range(group):
                    parts = [part[i * held : (i + 1) * held] for part in blocks]
                    lines.append(jnp.concatenate(parts, 0))
                for i in range(0, group, pair):
                    line = lines[i] if pair == 1 else jnp.concatenate(lines[i : i + pair], 1)
                    ready[g * (group // pair) + i // pair] = line

            if j >= SLOTS:
                y_left(c, j - SLOTS)
            elif count - SLOTS + j >= 0:
                @pl.when(c > 0)
                def _():
                    y_left(c - 1, count - SLOTS + j)

            @pl.loop(0, rows)
            def _(q):
                r = lax.rem(q + rows // 2, rows)
                peer = lax.rem(at_row + r, rows)
                for a in range(0, size, pair):
                    product = jnp.dot(
                        table_y[peer], ready[a // pair], preferred_element_type=jnp.float32
                    )
                    for g in range(pair):
                        by_cos = product[:y_local, g * width : (g + 1) * width]
                        by_sin = product[y_local:, g * width : (g + 1) * width]
                        swap = jnp.concatenate([-by_sin[:, half:], by_sin[:, :half]], 1)
                        total[:, a + g, :] = by_cos + swap
                if size < CHUNK:
                    total[:, size:, :] = jnp.zeros((y_local, CHUNK - size, width), jnp.float32)
                passed[j % SLOTS, peer] = total[...].astype(jnp.bfloat16)

                @pl.when(r == 0)
                def _():
                    y_own(c, j).start()

                @pl.when(r != 0)
                def _():
                    y_copy(c, j, r).start()

    @pl.loop(0, 3)
    def _(c):
        for j, (start, size) in enumerate(pieces):
            for r in range(1, cols):
                z_copy(c * count + j, r, size).wait_send()
            for r in range(1, rows):
                y_copy(c, j, r).wait_recv()

    for j in range(max(count - SLOTS, 0), count):
        y_left(2, j)


def gather(rows, cols, by_cos, by_sin, cos_y, sin_y, out_ref, mine, wide, tall, sums,
           send_c, recv_c, send_r, recv_r):
    at_col, at_row = lax.axis_index("col"), lax.axis_index("row")
    barrier = pltpu.get_barrier_semaphore()
    for r in range(1, cols):
        peer = lax.rem(at_col + r, cols)
        pl.semaphore_signal(barrier, inc=1, device_id={"col": peer}, device_id_type=MESH)
    for r in range(1, rows):
        peer = lax.rem(at_row + r, rows)
        pl.semaphore_signal(barrier, inc=1, device_id={"row": peer}, device_id_type=MESH)

    def swapped(value):
        half = value.shape[1] // 2
        return jnp.concatenate([value[:, half:], -value[:, :half]], 1)

    both = by_cos[...] + swapped(by_sin[...])
    both = both * cos_y[...] + swapped(both) * sin_y[...]
    mine[...] = jnp.broadcast_to(jnp.sum(both, 0, keepdims=True), mine.shape)
    pl.semaphore_wait(barrier, cols + rows - 2)

    def col_copy(r):
        return pltpu.make_async_remote_copy(
            src_ref=mine, dst_ref=wide.at[r], send_sem=send_c.at[r], recv_sem=recv_c.at[r],
            device_id={"col": lax.rem(at_col + r, cols)}, device_id_type=MESH)

    def row_copy(r):
        return pltpu.make_async_remote_copy(
            src_ref=sums, dst_ref=tall.at[r], send_sem=send_r.at[r], recv_sem=recv_r.at[r],
            device_id={"row": lax.rem(at_row + r, rows)}, device_id_type=MESH)

    for r in range(1, cols):
        col_copy(r).start()
    result = mine[...]
    for r in range(1, cols):
        col_copy(r).wait_recv()
        result = result + wide[r]
    sums[...] = result
    for r in range(1, rows):
        row_copy(r).start()
    for r in range(1, rows):
        row_copy(r).wait_recv()
        result = result + tall[r]
    out_ref[...] = result
    for r in range(1, cols):
        col_copy(r).wait_send()
    for r in range(1, rows):
        row_copy(r).wait_send()


def along_x(arrived_0, arrived_1, arrived_2, table_ref, phase_ref, weight_ref, cos_ref, sin_ref,
            velocity_ref, by_cos_ref, by_sin_ref, real_scr, imag_scr):
    ys, width = arrived_0.shape[2], arrived_0.shape[4]
    half = width // 2
    fields = []
    for c, arrived_ref in enumerate((arrived_0, arrived_1, arrived_2)):
        for y in range(ys):
            data = arrived_ref[:, 0, y].reshape(-1, width).T
            real_scr[c, y * half : (y + 1) * half, :] = data[:half]
            imag_scr[c, y * half : (y + 1) * half, :] = data[half:]
        field = jnp.dot(real_scr[c], table_ref[0], preferred_element_type=jnp.float32)
        field = field + jnp.dot(imag_scr[c], table_ref[1], preferred_element_type=jnp.float32)
        velocity_ref[c] = field.astype(jnp.bfloat16).reshape(velocity_ref.shape[1:])
        fields.append(field)
    f0, f1, f2 = fields
    trace = (f0 * f0 + f1 * f1 + f2 * f2) / 3.0
    stress = [f0 * f0 - trace, f1 * f1 - trace, f2 * f2 - trace, f0 * f1, f0 * f2, f1 * f2]
    mixed = None
    for index, part in enumerate(stress):
        line = jnp.dot(
            part.astype(jnp.bfloat16), phase_ref[...], preferred_element_type=jnp.float32
        )
        term = weight_ref[index : index + 1, :] * line
        mixed = term if mixed is None else mixed + term
    mixed = mixed.reshape(ys, half, -1)
    by_cos_ref[...] = jnp.sum(mixed * cos_ref[...][None], 1)
    by_sin_ref[...] = jnp.sum(mixed * sin_ref[...][None], 1)


def body(rows, cols, velocity_modes, wavenumbers, polar, azimuth):
    kx_local, ky_local, modes = velocity_modes.shape[1:]
    modes = modes // 2
    kx = kx_local * rows
    points = velocity_points(modes)
    y_local, z_local = points // rows, points // cols
    width = 2 * z_local
    kx_pad = padded(kx_local)

    group, held = grouping(kx_local, ky_local)
    pair = 2 if group % 2 == 0 and width % 128 == 0 else 1
    count = len(pieces_of(kx_local))
    table_z = z_table(modes, points, cols)
    table_y = y_table(modes, points, cols, rows, held)
    arrived = pl.pallas_call(
        functools.partial(exchange, rows, cols),
        in_specs=[
            pl.BlockSpec(memory_space=pl.ANY),
            pl.BlockSpec(memory_space=pltpu.VMEM),
            pl.BlockSpec(memory_space=pltpu.VMEM),
        ],
        out_specs=pl.BlockSpec(memory_space=pl.ANY),
        out_shape=jax.ShapeDtypeStruct((rows, 3, y_local, kx_pad, width), jnp.bfloat16),
        scratch_shapes=[
            pltpu.VMEM(velocity_modes.shape, jnp.bfloat16),
            pltpu.VMEM((3 * count, cols, CHUNK * held, width), jnp.bfloat16),
            pltpu.VMEM((3 * count, cols, CHUNK * held, width), jnp.bfloat16),
            pltpu.VMEM((CHUNK // pair, cols * held, pair * width), jnp.bfloat16),
            pltpu.VMEM((y_local, CHUNK, width), jnp.float32),
            pltpu.VMEM((SLOTS, rows, y_local, CHUNK, width), jnp.bfloat16),
            pltpu.SemaphoreType.DMA((3,)),
            pltpu.SemaphoreType.DMA((3 * count, cols)),
            pltpu.SemaphoreType.DMA((3 * count, cols)),
            pltpu.SemaphoreType.DMA((3, count, rows)),
            pltpu.SemaphoreType.DMA((3, count, rows)),
        ],
        compiler_params=pltpu.CompilerParams(
            vmem_limit_bytes=VMEM_LIMIT, collective_id=0, has_side_effects=True
        ),
        cost_estimate=estimate(3 * 2 * points, cols * ky_local, 2 * kx_local * width),
        name="exchange",
    )(velocity_modes, table_z, table_y)

    dirs, freqs = polar.shape[0], wavenumbers.shape[0]
    count_j = dirs * freqs
    wave_j = jnp.repeat(wavenumbers, dirs)
    axis_one = jnp.tile(jnp.sin(polar) * jnp.cos(azimuth), freqs)
    axis_two = jnp.tile(jnp.sin(polar) * jnp.sin(azimuth), freqs)
    axis_three = jnp.tile(jnp.cos(polar), freqs)
    unit = 2.0 * math.pi / points
    x_pos = jnp.arange(points, dtype=jnp.int32).astype(jnp.float32) * unit
    angle_x = wave_j[None, :] * (axis_one[None, :] * x_pos[:, None])
    phase_x = jnp.concatenate([jnp.cos(angle_x), -jnp.sin(angle_x)], 1).astype(jnp.bfloat16)
    weights = jnp.stack(
        [
            axis_one * axis_one,
            axis_two * axis_two,
            axis_three * axis_three,
            2.0 * axis_one * axis_two,
            2.0 * axis_one * axis_three,
            2.0 * axis_two * axis_three,
        ],
        0,
    )
    weights = jnp.concatenate([weights, weights], 1)
    z_index = lax.axis_index("col") * z_local + jnp.arange(z_local, dtype=jnp.int32)
    y_index = lax.axis_index("row") * y_local + jnp.arange(y_local, dtype=jnp.int32)
    angle_z = wave_j[None, :] * (axis_three[None, :] * (z_index.astype(jnp.float32) * unit)[:, None])
    angle_y = wave_j[None, :] * (axis_two[None, :] * (y_index.astype(jnp.float32) * unit)[:, None])
    cos_z, sin_z = jnp.cos(angle_z), jnp.sin(angle_z)

    ys = 8
    whole = lambda i: (0, 0)
    velocity, by_cos, by_sin = pl.pallas_call(
        along_x,
        grid=(y_local // ys,),
        in_specs=[
            *[
                pl.BlockSpec((rows, 1, ys, kx_pad, width), lambda i, c=c: (0, c, i, 0, 0))
                for c in range(3)
            ],
            pl.BlockSpec((2, rows * kx_pad, points), lambda i: (0, 0, 0)),
            pl.BlockSpec((points, 2 * count_j), whole),
            pl.BlockSpec((6, 2 * count_j), whole),
            pl.BlockSpec((z_local, 2 * count_j), whole),
            pl.BlockSpec((z_local, 2 * count_j), whole),
        ],
        out_specs=[
            pl.BlockSpec((3, ys, z_local, points), lambda i: (0, i, 0, 0)),
            pl.BlockSpec((ys, 2 * count_j), lambda i: (i, 0)),
            pl.BlockSpec((ys, 2 * count_j), lambda i: (i, 0)),
        ],
        out_shape=[
            jax.ShapeDtypeStruct((3, y_local, z_local, points), jnp.bfloat16),
            jax.ShapeDtypeStruct((y_local, 2 * count_j), jnp.float32),
            jax.ShapeDtypeStruct((y_local, 2 * count_j), jnp.float32),
        ],
        scratch_shapes=[pltpu.VMEM((3, ys * z_local, rows * kx_pad), jnp.bfloat16)] * 2,
        compiler_params=pltpu.CompilerParams(vmem_limit_bytes=VMEM_LIMIT),
        name="along_x",
    )(
        arrived,
        arrived,
        arrived,
        x_table(kx, points, rows),
        phase_x,
        weights,
        jnp.concatenate([cos_z, cos_z], 1),
        jnp.concatenate([sin_z, sin_z], 1),
    )
    cos_y, sin_y = jnp.cos(angle_y), jnp.sin(angle_y)
    peers = lambda n: pltpu.SemaphoreType.DMA((n,))
    tile = (8, 2 * count_j)
    terms = pl.pallas_call(
        functools.partial(gather, rows, cols),
        in_specs=[pl.BlockSpec(memory_space=pltpu.VMEM)] * 4,
        out_specs=pl.BlockSpec(memory_space=pltpu.VMEM),
        out_shape=jax.ShapeDtypeStruct(tile, jnp.float32),
        scratch_shapes=[
            pltpu.VMEM(tile, jnp.float32),
            pltpu.VMEM((cols, *tile), jnp.float32),
            pltpu.VMEM((rows, *tile), jnp.float32),
            pltpu.VMEM(tile, jnp.float32),
            peers(cols), peers(cols), peers(rows), peers(rows),
        ],
        compiler_params=pltpu.CompilerParams(collective_id=1, has_side_effects=True),
        name="gather",
    )(by_cos, by_sin, jnp.concatenate([cos_y, cos_y], 1), jnp.concatenate([sin_y, sin_y], 1))
    spectrum = terms[0].reshape(2, freqs, dirs) * (wavenumbers * wavenumbers)[None, :, None]
    total = jnp.transpose(spectrum / points**1.5, (2, 0, 1))
    owned = dirs // cols
    far_field = lax.dynamic_slice_in_dim(total, lax.axis_index("col") * owned, owned, 0)
    return (velocity, far_field)


def velocity_points(modes):
    return 1 << (modes - 1).bit_length()


def solution(mesh):
    return jax.shard_map(
        functools.partial(body, mesh.shape["row"], mesh.shape["col"]),
        mesh=mesh,
        in_specs=(P(None, "row", "col", None), P(), P(), P()),
        out_specs=(P(None, "row", "col", None), P("col", None, None)),
        check_vma=False,
    )
```

```python
import functools
import math

import jax
import jax.numpy as jnp
import numpy as np
from jax import lax
from jax.experimental import pallas as pl
from jax.experimental.pallas import tpu as pltpu
from jax.sharding import PartitionSpec as P

VMEM_LIMIT = 60 * 1024 * 1024


def padded(count):
    return -(-count // 16) * 16


def lanes(count):
    return -(-count // 128) * 128


def circle(waves, cells, points):
    angle = np.mod(np.outer(waves, cells), points).astype(np.float64) * (2.0 * math.pi / points)
    return np.cos(angle).astype(np.float32), np.sin(angle).astype(np.float32)


def z_table(modes, points, blocks):
    cosine, sine = circle(np.arange(modes) - modes // 2, np.arange(points), points)
    cosine, sine = (part.reshape(modes, blocks, 1, -1) for part in (cosine, sine))
    table = np.concatenate(
        [np.concatenate([cosine, sine], 2), np.concatenate([-sine, cosine], 2)], 0
    )
    return jnp.asarray(table.reshape(2 * modes, 2 * points).astype(jnp.bfloat16))


def estimate(rows, depth, columns):
    return pl.CostEstimate(
        flops=2 * rows * depth * columns,
        bytes_accessed=2 * (rows * depth + depth * columns + rows * columns),
        transcendentals=0,
    )


MESH = pl.DeviceIdType.MESH
CHUNK = 8
SLOTS = 3
WINDOW = 2


def grouping(kx, ky):
    if kx % 4 == 0 and ky % 4 == 0:
        return 4, ky
    return 1, padded(ky)


def pieces_of(kx):
    first = kx % CHUNK or CHUNK
    starts = [0, *range(first, kx, CHUNK)]
    return [(start, CHUNK if start else first) for start in starts]


def spread(ref, inner, shape):
    lane = lax.broadcasted_iota(jnp.int32, shape, 1)
    count = ref.shape[0]
    total = jnp.zeros(shape, jnp.float32)
    for start in range(0, shape[1], inner):
        here = jnp.logical_and(lane >= start, lane < start + inner)
        total = jnp.where(here, ref[(start // inner) % count], total)
    return total


def turn(waves, cells, points):
    product = jnp.bitwise_and(waves * cells, points - 1)
    return product.astype(jnp.float32) * (2.0 * math.pi / points)


def y_tables(table_y, held, ky):
    blocks, double, depth = table_y.shape
    cells = double // 2
    points = blocks * cells
    modes = depth // held * ky
    tile = min(cells, 64)

    @pl.loop(0, points // tile)
    def _(i):
        shape = (tile, depth)
        lane = lax.broadcasted_iota(jnp.int32, shape, 1)
        source = jnp.floor((lane.astype(jnp.float32) + 0.5) / held).astype(jnp.int32)
        slot = lane - source * held
        cell = lax.broadcasted_iota(jnp.int32, shape, 0) + i * tile
        angle = turn(source * ky + slot - modes // 2, cell, points)
        block = i // (cells // tile)
        at = pl.multiple_of(lax.rem(i, cells // tile) * tile, tile)
        for base, part in ((0, jnp.cos(angle)), (cells, jnp.sin(angle))):
            part = jnp.where(slot < ky, part, 0.0).astype(jnp.bfloat16)
            table_y[block, pl.ds(base + at, tile), :] = part


def x_tables(table_x, rows, kx):
    depth, points = table_x.shape[0] // 2, table_x.shape[1]
    held = padded(kx)
    first = pieces_of(kx)[0][1]
    table_x[...] = jnp.zeros_like(table_x)

    @pl.loop(0, rows)
    def _(source):
        shape = (held, points)
        slot = lax.broadcasted_iota(jnp.int32, shape, 0)
        local = jnp.where(slot < first, slot, slot - (CHUNK - first))
        keep = jnp.logical_and(
            jnp.logical_or(slot < first, slot >= CHUNK), local < kx
        )
        wave = source * kx + local
        angle = turn(wave, lax.broadcasted_iota(jnp.int32, shape, 1), points)
        factor = jnp.where(keep, jnp.where(wave == 0, 1.0, 2.0), 0.0)
        for base, part in ((0, jnp.cos(angle)), (depth, -jnp.sin(angle))):
            part = factor * part.astype(jnp.bfloat16).astype(jnp.float32)
            at = pl.ds(pl.multiple_of(base + source * held, 16), held)
            table_x[at, :] = part.astype(jnp.bfloat16)


def phases(wave_ref, polar_ref, azimuth_ref, phase_ref, weight_ref, z_ref, y_ref, at_col, at_row):
    points, count = phase_ref.shape
    dirs = polar_ref.shape[0]
    row = (1, count)
    wave = spread(wave_ref, dirs, row)
    polar, azimuth = spread(polar_ref, 1, row), spread(azimuth_ref, 1, row)
    one = jnp.sin(polar) * jnp.cos(azimuth)
    two = jnp.sin(polar) * jnp.sin(azimuth)
    three = jnp.cos(polar)
    unit = 2.0 * math.pi / points

    def angle(axis, first, shape):
        at = lax.broadcasted_iota(jnp.int32, shape, 0) + first
        return wave * (axis * (at.astype(jnp.float32) * unit))

    square = [one * one, two * two, three * three]
    weights = [
        (2.0 * square[0] - square[1] - square[2]) / 3.0,
        (2.0 * square[1] - square[0] - square[2]) / 3.0,
        2.0 * one * two,
        2.0 * one * three,
        2.0 * two * three,
    ]
    for index, weight in enumerate(weights):
        weight_ref[index : index + 1, :] = weight
    weight_ref[5:8, :] = jnp.zeros((3, count), jnp.float32)
    tile = min(points, 64)

    @pl.loop(0, points // tile)
    def _(i):
        shape = (tile, count)
        at = angle(one, i * tile, shape)
        real = lax.broadcasted_iota(jnp.int32, shape, 1) < count // 2
        phase = jnp.where(real, jnp.cos(at), -jnp.sin(at))
        phase_ref[pl.ds(pl.multiple_of(i * tile, tile), tile), :] = phase.astype(jnp.bfloat16)

    for ref, axis, where, scale in (
        (z_ref, three, at_col, 1.0),
        (y_ref, two, at_row, wave * wave / points**1.5),
    ):
        held = ref.shape[1]
        at = angle(axis, where * held, (held, count))
        ref[0] = jnp.cos(at) * scale
        ref[1] = jnp.sin(at) * scale


def exchange(rows, cols, modes_ref, table_z, wave_ref, polar_ref, azimuth_ref,
             out_ref, table_x, phase_ref, weight_ref, z_ref, y_ref, table_y, modes, sent, came, ready, total, passed,
             in_sem, send_z, recv_z, send_y, recv_y):
    kx, ky = modes.shape[1], modes.shape[2]
    width = came.shape[3]
    half = width // 2
    y_local = out_ref.shape[2]
    at_col, at_row = lax.axis_index("col"), lax.axis_index("row")
    group, held = grouping(kx, ky)
    block = group * held
    pieces = pieces_of(kx)
    count = len(pieces)
    pair = ready.shape[2] // width

    def load(c):
        return pltpu.make_async_copy(modes_ref.at[c], modes.at[c], in_sem.at[c])

    for c in range(3):
        load(c).start()
    barrier = pltpu.get_barrier_semaphore()
    for r in range(1, cols):
        peer = lax.rem(at_col + r, cols)
        pl.semaphore_signal(barrier, inc=1, device_id={"col": peer}, device_id_type=MESH)
    for r in range(1, rows):
        peer = lax.rem(at_row + r, rows)
        pl.semaphore_signal(barrier, inc=1, device_id={"row": peer}, device_id_type=MESH)

    def z_copy(c, j, r):
        t = c * count + j
        peer = lax.rem(at_col + r, cols)
        used = pl.ds(0, pieces[j][1] * held)
        return pltpu.make_async_remote_copy(
            src_ref=sent.at[j, peer, used], dst_ref=came.at[t, at_col, used],
            send_sem=send_z.at[t, r], recv_sem=recv_z.at[t, r],
            device_id={"col": peer}, device_id_type=MESH)

    def y_copy(c, j, r):
        peer = lax.rem(at_row + r, rows)
        return pltpu.make_async_remote_copy(
            src_ref=passed.at[j % SLOTS, peer],
            dst_ref=out_ref.at[at_row, c, :, pl.ds(j * CHUNK, CHUNK), :],
            send_sem=send_y.at[c, j, r], recv_sem=recv_y.at[c, j, r],
            device_id={"row": peer}, device_id_type=MESH)

    def y_own(c, j):
        return pltpu.make_async_copy(
            passed.at[j % SLOTS, at_row],
            out_ref.at[at_row, c, :, pl.ds(j * CHUNK, CHUNK), :], send_y.at[c, j, 0])

    def y_left(c, j):
        y_own(c, j).wait()
        for r in range(1, rows):
            y_copy(c, j, r).wait_send()

    def z_make(c, j):
        start, size = pieces[j]
        t = c * count + j
        if j == 0:
            load(c).wait()

        @pl.loop(0, size // group)
        def _(g):
            slabs = [modes[c, start + g * group + i] for i in range(group)]
            data = slabs[0] if group == 1 else jnp.concatenate(slabs, 0)
            value = jnp.dot(data, table_z[...], preferred_element_type=jnp.float32)
            value = value.astype(jnp.bfloat16)
            if value.shape[0] < block:
                spare = jnp.zeros((block - value.shape[0], value.shape[1]), jnp.bfloat16)
                value = jnp.concatenate([value, spare], 0)
            at = pl.ds(pl.multiple_of(g * block, 16), block)
            for b in range(cols):
                sent[j, b, at, :] = value[:, b * width : (b + 1) * width]
            came[t, at_col, at, :] = sent[j, at_col, at, :]

    def z_start(c, j):
        for r in range(1, cols):
            z_copy(c, j, r).start()

    def ahead(c, j):
        return (c, j) if j < count else ahead(c + 1, j - count)

    total[...] = jnp.zeros_like(total)
    for u in range(min(WINDOW, 3 * count)):
        c, j = ahead(0, u)
        z_make(c, j)
        if u == 0:
            pl.semaphore_wait(barrier, cols + rows - 2)
        z_start(c, j)
    y_tables(table_y, held, ky)
    x_tables(table_x, rows, kx)
    phases(wave_ref, polar_ref, azimuth_ref, phase_ref, weight_ref, z_ref, y_ref, at_col, at_row)

    @pl.loop(0, 3)
    def _(c):
        for j, (start, size) in enumerate(pieces):
            t = c * count + j
            c_next, j_next = ahead(c, j + WINDOW)
            later = j + WINDOW >= count

            def make():
                if later:
                    for r in range(1, cols):
                        z_copy(c_next - 1, j_next, r).wait_send()
                else:
                    @pl.when(c > 0)
                    def _():
                        for r in range(1, cols):
                            z_copy(c - 1, j_next, r).wait_send()
                z_make(c_next, j_next)

            if later:
                pl.when(c_next < 3)(make)
            else:
                make()
            for r in range(1, cols):
                z_copy(c, j, r).wait_recv()
            if later:
                pl.when(c_next < 3)(functools.partial(z_start, c_next, j_next))
            else:
                z_start(c_next, j_next)

            @pl.loop(0, size // group)
            def _(g):
                at = pl.ds(pl.multiple_of(g * block, 16), block)
                blocks = [came[t, s, at, :] for s in range(cols)]
                lines = []
                for i in range(group):
                    parts = [part[i * held : (i + 1) * held] for part in blocks]
                    lines.append(jnp.concatenate(parts, 0))
                for i in range(0, group, pair):
                    line = lines[i] if pair == 1 else jnp.concatenate(lines[i : i + pair], 1)
                    ready[g * (group // pair) + i // pair] = line

            if j >= SLOTS:
                y_left(c, j - SLOTS)
            elif count - SLOTS + j >= 0:
                @pl.when(c > 0)
                def _():
                    y_left(c - 1, count - SLOTS + j)

            @pl.loop(0, rows)
            def _(q):
                step = jnp.where(lax.rem(at_row, 2) == 0, q, rows - q)
                r = lax.rem(step + rows // 2, rows)
                peer = lax.rem(at_row + r, rows)
                for a in range(0, size, pair):
                    product = jnp.dot(
                        table_y[peer], ready[a // pair], preferred_element_type=jnp.float32
                    )
                    for g in range(pair):
                        by_cos = product[:y_local, g * width : (g + 1) * width]
                        by_sin = product[y_local:, g * width : (g + 1) * width]
                        swap = jnp.concatenate([-by_sin[:, half:], by_sin[:, :half]], 1)
                        total[:, a + g, :] = by_cos + swap
                if size < CHUNK:
                    total[:, size:, :] = jnp.zeros((y_local, CHUNK - size, width), jnp.float32)
                passed[j % SLOTS, peer] = total[...].astype(jnp.bfloat16)

                @pl.when(r == 0)
                def _():
                    y_own(c, j).start()

                @pl.when(r != 0)
                def _():
                    y_copy(c, j, r).start()

    @pl.loop(0, 3)
    def _(c):
        for j, (start, size) in enumerate(pieces):
            for r in range(1, rows):
                y_copy(c, j, r).wait_recv()

    for j in range(count):
        for r in range(1, cols):
            z_copy(2, j, r).wait_send()
    for j in range(max(count - SLOTS, 0), count):
        y_left(2, j)


def gather(rows, cols, freqs, by_cos, by_sin, y_ref, out_ref, mine, wide, tall, sums,
           send_c, recv_c, send_r, recv_r):
    at_col, at_row = lax.axis_index("col"), lax.axis_index("row")
    barrier = pltpu.get_barrier_semaphore()
    for r in range(1, cols):
        peer = lax.rem(at_col + r, cols)
        pl.semaphore_signal(barrier, inc=1, device_id={"col": peer}, device_id_type=MESH)
    for r in range(1, rows):
        peer = lax.rem(at_row + r, rows)
        pl.semaphore_signal(barrier, inc=1, device_id={"row": peer}, device_id_type=MESH)

    def swapped(value):
        half = value.shape[1] // 2
        return jnp.concatenate([value[:, half:], -value[:, :half]], 1)

    both = by_cos[...] + swapped(by_sin[...])
    both = both * y_ref[0] + swapped(both) * y_ref[1]
    mine[...] = jnp.broadcast_to(jnp.sum(both, 0, keepdims=True), mine.shape)
    pl.semaphore_wait(barrier, cols + rows - 2)

    def col_copy(r):
        return pltpu.make_async_remote_copy(
            src_ref=mine, dst_ref=wide.at[r], send_sem=send_c.at[r], recv_sem=recv_c.at[r],
            device_id={"col": lax.rem(at_col + r, cols)}, device_id_type=MESH)

    def row_copy(r):
        return pltpu.make_async_remote_copy(
            src_ref=sums, dst_ref=tall.at[r], send_sem=send_r.at[r], recv_sem=recv_r.at[r],
            device_id={"row": lax.rem(at_row + r, rows)}, device_id_type=MESH)

    for r in range(1, cols):
        col_copy(r).start()
    result = mine[...]
    for r in range(1, cols):
        col_copy(r).wait_recv()
        result = result + wide[r]
    sums[...] = result
    for r in range(1, rows):
        row_copy(r).start()
    for r in range(1, rows):
        row_copy(r).wait_recv()
        result = result + tall[r]
    count = result.shape[1]
    dirs = count // (2 * freqs)
    lane = lax.broadcasted_iota(jnp.int32, result.shape, 1)
    part = lax.broadcasted_iota(jnp.int32, result.shape, 0)
    result = jnp.where((lane >= count // 2) == (part == 1), result, 0.0)
    shape = (count // 2, freqs)
    place = lax.broadcasted_iota(jnp.int32, shape, 0)
    freq = lax.broadcasted_iota(jnp.int32, shape, 1)
    for own in range(out_ref.shape[0]):
        direction = at_col * out_ref.shape[0] + own
        pick = jnp.where(place == freq * dirs + direction, 1.0, 0.0)
        pick = jnp.concatenate([pick, pick], 0)
        out_ref[own] = jnp.dot(
            result, pick, precision=lax.Precision.HIGHEST, preferred_element_type=jnp.float32
        )[:2]
    for r in range(1, cols):
        col_copy(r).wait_send()
    for r in range(1, rows):
        row_copy(r).wait_send()


def along_x(arrived_0, arrived_1, arrived_2, table_ref, phase_ref, weight_ref, z_ref,
            velocity_ref, by_cos_ref, by_sin_ref, real_scr, imag_scr):
    ys, width = arrived_0.shape[2], arrived_0.shape[4]
    half = width // 2
    held = real_scr.shape[2]
    depth = table_ref.shape[0] // 2
    fields = []
    for c, arrived_ref in enumerate((arrived_0, arrived_1, arrived_2)):
        for y in range(ys):
            data = arrived_ref[:, 0, y].reshape(-1, width).T
            real_scr[c, y * half : (y + 1) * half, :] = data[:half]
            imag_scr[c, y * half : (y + 1) * half, :] = data[half:]
        field = jnp.dot(real_scr[c], table_ref[0:held], preferred_element_type=jnp.float32)
        field = field + jnp.dot(
            imag_scr[c], table_ref[depth : depth + held], preferred_element_type=jnp.float32
        )
        velocity_ref[c] = field.astype(jnp.bfloat16).reshape(velocity_ref.shape[1:])
        fields.append(field)
    f0, f1, f2 = fields
    last = f2 * f2
    stress = [f0 * f0 - last, f1 * f1 - last, f0 * f1, f0 * f2, f1 * f2]
    mixed = None
    for index, part in enumerate(stress):
        line = jnp.dot(
            part.astype(jnp.bfloat16), phase_ref[...], preferred_element_type=jnp.float32
        )
        term = weight_ref[index : index + 1, :] * line
        mixed = term if mixed is None else mixed + term
    mixed = mixed.reshape(ys, half, -1)
    by_cos_ref[...] = jnp.sum(mixed * z_ref[0][None], 1)
    by_sin_ref[...] = jnp.sum(mixed * z_ref[1][None], 1)


def body(rows, cols, velocity_modes, wavenumbers, polar, azimuth):
    kx_local, ky_local, modes = velocity_modes.shape[1:]
    modes = modes // 2
    points = velocity_points(modes)
    y_local, z_local = points // rows, points // cols
    width = 2 * z_local
    kx_pad = padded(kx_local)

    group, held = grouping(kx_local, ky_local)
    pair = 2 if group % 2 == 0 and width % 128 == 0 else 1
    count = len(pieces_of(kx_local))
    dirs, freqs = polar.shape[0], wavenumbers.shape[0]
    width_j = 2 * dirs * freqs
    depth = lanes(rows * kx_pad)
    table_z = z_table(modes, points, cols)
    arrived, table_x, phase, weights, near_z, near_y = pl.pallas_call(
        functools.partial(exchange, rows, cols),
        in_specs=[
            pl.BlockSpec(memory_space=pl.ANY),
            pl.BlockSpec(memory_space=pltpu.VMEM),
            *[pl.BlockSpec(memory_space=pltpu.SMEM)] * 3,
        ],
        out_specs=[
            pl.BlockSpec(memory_space=pl.ANY),
            *[pl.BlockSpec(memory_space=pltpu.VMEM)] * 5,
        ],
        out_shape=[
            jax.ShapeDtypeStruct((rows, 3, y_local, kx_pad, width), jnp.bfloat16),
            jax.ShapeDtypeStruct((2 * depth, points), jnp.bfloat16),
            jax.ShapeDtypeStruct((points, width_j), jnp.bfloat16),
            jax.ShapeDtypeStruct((8, width_j), jnp.float32),
            jax.ShapeDtypeStruct((2, z_local, width_j), jnp.float32),
            jax.ShapeDtypeStruct((2, y_local, width_j), jnp.float32),
        ],
        scratch_shapes=[
            pltpu.VMEM((rows, 2 * y_local, cols * held), jnp.bfloat16),
            pltpu.VMEM(velocity_modes.shape, jnp.bfloat16),
            pltpu.VMEM((count, cols, CHUNK * held, width), jnp.bfloat16),
            pltpu.VMEM((3 * count, cols, CHUNK * held, width), jnp.bfloat16),
            pltpu.VMEM((CHUNK // pair, cols * held, pair * width), jnp.bfloat16),
            pltpu.VMEM((y_local, CHUNK, width), jnp.float32),
            pltpu.VMEM((SLOTS, rows, y_local, CHUNK, width), jnp.bfloat16),
            pltpu.SemaphoreType.DMA((3,)),
            pltpu.SemaphoreType.DMA((3 * count, cols)),
            pltpu.SemaphoreType.DMA((3 * count, cols)),
            pltpu.SemaphoreType.DMA((3, count, rows)),
            pltpu.SemaphoreType.DMA((3, count, rows)),
        ],
        compiler_params=pltpu.CompilerParams(
            vmem_limit_bytes=VMEM_LIMIT, collective_id=0, has_side_effects=True
        ),
        cost_estimate=estimate(3 * 2 * points, cols * ky_local, 2 * kx_local * width),
        name="exchange",
    )(velocity_modes, table_z, wavenumbers, polar, azimuth)

    ys = 16
    whole = lambda i: (0, 0)
    velocity, by_cos, by_sin = pl.pallas_call(
        along_x,
        grid=(y_local // ys,),
        in_specs=[
            *[
                pl.BlockSpec((rows, 1, ys, kx_pad, width), lambda i, c=c: (0, c, i, 0, 0))
                for c in range(3)
            ],
            pl.BlockSpec((2 * depth, points), whole),
            pl.BlockSpec((points, width_j), whole),
            pl.BlockSpec((8, width_j), whole),
            pl.BlockSpec((2, z_local, width_j), lambda i: (0, 0, 0)),
        ],
        out_specs=[
            pl.BlockSpec((3, ys, z_local, points), lambda i: (0, i, 0, 0)),
            pl.BlockSpec((ys, width_j), lambda i: (i, 0)),
            pl.BlockSpec((ys, width_j), lambda i: (i, 0)),
        ],
        out_shape=[
            jax.ShapeDtypeStruct((3, y_local, z_local, points), jnp.bfloat16),
            jax.ShapeDtypeStruct((y_local, width_j), jnp.float32),
            jax.ShapeDtypeStruct((y_local, width_j), jnp.float32),
        ],
        scratch_shapes=[
            pltpu.VMEM((3, ys * z_local, rows * kx_pad), jnp.bfloat16),
            pltpu.VMEM((3, ys * z_local, rows * kx_pad), jnp.bfloat16),
        ],
        compiler_params=pltpu.CompilerParams(vmem_limit_bytes=VMEM_LIMIT),
        name="along_x",
    )(
        arrived,
        arrived,
        arrived,
        table_x,
        phase,
        weights,
        near_z,
    )
    peers = lambda n: pltpu.SemaphoreType.DMA((n,))
    tile = (8, width_j)
    far_field = pl.pallas_call(
        functools.partial(gather, rows, cols, freqs),
        in_specs=[pl.BlockSpec(memory_space=pltpu.VMEM)] * 3,
        out_specs=pl.BlockSpec(memory_space=pltpu.VMEM),
        out_shape=jax.ShapeDtypeStruct((dirs // cols, 2, freqs), jnp.float32),
        scratch_shapes=[
            pltpu.VMEM(tile, jnp.float32),
            pltpu.VMEM((cols, *tile), jnp.float32),
            pltpu.VMEM((rows, *tile), jnp.float32),
            pltpu.VMEM(tile, jnp.float32),
            peers(cols), peers(cols), peers(rows), peers(rows),
        ],
        compiler_params=pltpu.CompilerParams(collective_id=1, has_side_effects=True),
        name="gather",
    )(by_cos, by_sin, near_y)
    return (velocity, far_field)


def velocity_points(modes):
    return 1 << (modes - 1).bit_length()


def solution(mesh):
    return jax.shard_map(
        functools.partial(body, mesh.shape["row"], mesh.shape["col"]),
        mesh=mesh,
        in_specs=(P(None, "row", "col", None), P(), P(), P()),
        out_specs=(P(None, "row", "col", None), P("col", None, None)),
        check_vma=False,
    )
```

```python
import functools
import math

import jax
import jax.numpy as jnp
import numpy as np
from jax import lax
from jax.experimental import pallas as pl
from jax.experimental.pallas import tpu as pltpu
from jax.sharding import PartitionSpec as P

VMEM_LIMIT = 60 * 1024 * 1024


def padded(count):
    return -(-count // 16) * 16


def lanes(count):
    return -(-count // 128) * 128


def circle(waves, cells, points):
    angle = np.mod(np.outer(waves, cells), points).astype(np.float64) * (2.0 * math.pi / points)
    return np.cos(angle).astype(np.float32), np.sin(angle).astype(np.float32)


def z_table(modes, points, blocks):
    cosine, sine = circle(np.arange(modes) - modes // 2, np.arange(points), points)
    cosine, sine = (part.reshape(modes, blocks, 1, -1) for part in (cosine, sine))
    table = np.concatenate(
        [np.concatenate([cosine, sine], 2), np.concatenate([-sine, cosine], 2)], 0
    )
    return jnp.asarray(table.reshape(2 * modes, 2 * points).astype(jnp.bfloat16))


def estimate(rows, depth, columns):
    return pl.CostEstimate(
        flops=2 * rows * depth * columns,
        bytes_accessed=2 * (rows * depth + depth * columns + rows * columns),
        transcendentals=0,
    )


MESH = pl.DeviceIdType.MESH
CHUNK = 8
SLOTS = 3
WINDOW = 2


def grouping(kx, ky):
    if kx % 4 == 0 and ky % 4 == 0:
        return 4, ky
    return 1, padded(ky)


def pieces_of(kx):
    first = kx % CHUNK or CHUNK
    starts = [0, *range(first, kx, CHUNK)]
    return [(start, CHUNK if start else first) for start in starts]


def spread(ref, inner, shape):
    lane = lax.broadcasted_iota(jnp.int32, shape, 1)
    count = ref.shape[0]
    total = jnp.zeros(shape, jnp.float32)
    for start in range(0, shape[1], inner):
        here = jnp.logical_and(lane >= start, lane < start + inner)
        total = jnp.where(here, ref[(start // inner) % count], total)
    return total


def turn(waves, cells, points):
    product = jnp.bitwise_and(waves * cells, points - 1)
    return product.astype(jnp.float32) * (2.0 * math.pi / points)


def y_tables(table_y, held, ky):
    blocks, double, depth = table_y.shape
    cells = double // 2
    points = blocks * cells
    modes = depth // held * ky
    tile = min(cells, 64)

    @pl.loop(0, points // tile)
    def _(i):
        shape = (tile, depth)
        lane = lax.broadcasted_iota(jnp.int32, shape, 1)
        source = jnp.floor((lane.astype(jnp.float32) + 0.5) / held).astype(jnp.int32)
        slot = lane - source * held
        cell = lax.broadcasted_iota(jnp.int32, shape, 0) + i * tile
        angle = turn(source * ky + slot - modes // 2, cell, points)
        block = i // (cells // tile)
        at = pl.multiple_of(lax.rem(i, cells // tile) * tile, tile)
        for base, part in ((0, jnp.cos(angle)), (cells, jnp.sin(angle))):
            part = jnp.where(slot < ky, part, 0.0).astype(jnp.bfloat16)
            table_y[block, pl.ds(base + at, tile), :] = part


def x_tables(table_x, rows, kx):
    depth, points = table_x.shape[0] // 2, table_x.shape[1]
    held = padded(kx)
    first = pieces_of(kx)[0][1]
    table_x[...] = jnp.zeros_like(table_x)

    @pl.loop(0, rows)
    def _(source):
        shape = (held, points)
        slot = lax.broadcasted_iota(jnp.int32, shape, 0)
        local = jnp.where(slot < first, slot, slot - (CHUNK - first))
        keep = jnp.logical_and(
            jnp.logical_or(slot < first, slot >= CHUNK), local < kx
        )
        wave = source * kx + local
        angle = turn(wave, lax.broadcasted_iota(jnp.int32, shape, 1), points)
        factor = jnp.where(keep, jnp.where(wave == 0, 1.0, 2.0), 0.0)
        for base, part in ((0, jnp.cos(angle)), (depth, -jnp.sin(angle))):
            part = factor * part.astype(jnp.bfloat16).astype(jnp.float32)
            at = pl.ds(pl.multiple_of(base + source * held, 16), held)
            table_x[at, :] = part.astype(jnp.bfloat16)


def phases(wave_ref, polar_ref, azimuth_ref, phase_ref, weight_ref, z_ref, y_ref, at_col, at_row):
    points, count = phase_ref.shape
    dirs = polar_ref.shape[0]
    row = (1, count)
    wave = spread(wave_ref, dirs, row)
    polar, azimuth = spread(polar_ref, 1, row), spread(azimuth_ref, 1, row)
    one = jnp.sin(polar) * jnp.cos(azimuth)
    two = jnp.sin(polar) * jnp.sin(azimuth)
    three = jnp.cos(polar)
    unit = 2.0 * math.pi / points

    def angle(axis, first, shape):
        at = lax.broadcasted_iota(jnp.int32, shape, 0) + first
        return wave * (axis * (at.astype(jnp.float32) * unit))

    square = [one * one, two * two, three * three]
    trace = (square[0] + square[1] + square[2]) / 3.0
    weights = [
        square[0] - trace,
        square[1] - trace,
        2.0 * one * two,
        square[2] - trace,
        2.0 * one * three,
        2.0 * two * three,
    ]
    for index, weight in enumerate(weights):
        weight_ref[index : index + 1, :] = weight
    weight_ref[6:8, :] = jnp.zeros((2, count), jnp.float32)
    tile = min(points, 64)

    @pl.loop(0, points // tile)
    def _(i):
        shape = (tile, count)
        at = angle(one, i * tile, shape)
        real = lax.broadcasted_iota(jnp.int32, shape, 1) < count // 2
        phase = jnp.where(real, jnp.cos(at), -jnp.sin(at))
        phase_ref[pl.ds(pl.multiple_of(i * tile, tile), tile), :] = phase.astype(jnp.bfloat16)

    for ref, axis, where, scale in (
        (z_ref, three, at_col, 1.0),
        (y_ref, two, at_row, wave * wave / points**1.5),
    ):
        held = ref.shape[1]
        at = angle(axis, where * held, (held, count))
        ref[0] = jnp.cos(at) * scale
        ref[1] = jnp.sin(at) * scale


def x_field(real, imag, table_ref):
    held, depth = real.shape[1], table_ref.shape[0] // 2
    field = jnp.dot(real, table_ref[0:held], preferred_element_type=jnp.float32)
    return field + jnp.dot(
        imag, table_ref[depth : depth + held], preferred_element_type=jnp.float32
    )


def x_lines(stress, first, phase_ref, weight_ref, z_ref, ys):
    mixed = None
    for index, part in enumerate(stress):
        line = jnp.dot(
            part.astype(jnp.bfloat16), phase_ref[...], preferred_element_type=jnp.float32
        )
        term = weight_ref[first + index : first + index + 1, :] * line
        mixed = term if mixed is None else mixed + term
    mixed = mixed.reshape(ys, -1, mixed.shape[1])
    return jnp.sum(mixed * z_ref[0][None], 1), jnp.sum(mixed * z_ref[1][None], 1)


def exchange(rows, cols, modes_ref, table_z, wave_ref, polar_ref, azimuth_ref,
             out_ref, early_ref, early_cos, early_sin, table_x, phase_ref, weight_ref, z_ref, y_ref,
             x_in, x_real, x_imag, x_out, in_x, out_x, table_y, modes, sent, came, ready, total, passed,
             in_sem, send_z, recv_z, send_y, recv_y):
    kx, ky = modes.shape[1], modes.shape[2]
    width = came.shape[3]
    half = width // 2
    y_local = out_ref.shape[2]
    at_col, at_row = lax.axis_index("col"), lax.axis_index("row")
    group, held = grouping(kx, ky)
    block = group * held
    pieces = pieces_of(kx)
    count = len(pieces)
    pair = ready.shape[2] // width
    slots = passed.shape[0]
    ys = x_in.shape[3]
    y_blocks = y_local // ys

    def x_load(b, e):
        slot = lax.rem(b, 2)
        at = pl.ds(pl.multiple_of(b * ys, ys), ys)
        return pltpu.make_async_copy(
            out_ref.at[:, e, at], x_in.at[slot, e], in_x.at[slot, e])

    def x_store(b, e):
        slot = lax.rem(b, 2)
        at = pl.ds(pl.multiple_of(b * ys, ys), ys)
        return pltpu.make_async_copy(
            x_out.at[slot, e], early_ref.at[e, at], out_x.at[slot, e])

    def x_run(low, high):
        for e in range(2):
            x_load(low, e).start()

        @pl.loop(low, high)
        def _(b):
            slot = lax.rem(b, 2)

            @pl.when(b + 1 < high)
            def _():
                for e in range(2):
                    x_load(b + 1, e).start()

            for e in range(2):
                x_load(b, e).wait()

            @pl.when(b >= low + 2)
            def _():
                for e in range(2):
                    x_store(b - 2, e).wait()

            fields = []
            for e in range(2):
                for y in range(ys):
                    data = x_in[slot, e, :, y].reshape(-1, width).T
                    x_real[e, y * half : (y + 1) * half, :] = data[:half]
                    x_imag[e, y * half : (y + 1) * half, :] = data[half:]
                field = x_field(x_real[e], x_imag[e], table_x)
                x_out[slot, e] = field.astype(jnp.bfloat16).reshape(x_out.shape[2:])
                fields.append(field)
            for e in range(2):
                x_store(b, e).start()
            f0, f1 = fields
            at = pl.ds(pl.multiple_of(b * ys, ys), ys)
            early_cos[at, :], early_sin[at, :] = x_lines(
                [f0 * f0, f1 * f1, f0 * f1], 0, phase_ref, weight_ref, z_ref, ys
            )

        for b in range(max(low, high - 2), high):
            for e in range(2):
                x_store(b, e).wait()

    middle = count // 2
    if middle < slots - 1 or middle >= count - 1 or y_blocks % 2:
        middle = None
    share = y_blocks // 2 if middle is not None else 0

    def x_early(j):
        if j == (count - 1 if middle is None else middle):
            for c in range(2):
                for i in range(count):
                    for r in range(1, rows):
                        y_copy(c, i, r).wait_recv()
        if j == middle:
            x_run(0, share)
        if j == count - 1:
            x_run(share, y_blocks)

    def load(c):
        return pltpu.make_async_copy(modes_ref.at[c], modes.at[c], in_sem.at[c])

    for c in range(3):
        load(c).start()
    barrier = pltpu.get_barrier_semaphore()
    for r in range(1, cols):
        peer = lax.rem(at_col + r, cols)
        pl.semaphore_signal(barrier, inc=1, device_id={"col": peer}, device_id_type=MESH)
    for r in range(1, rows):
        peer = lax.rem(at_row + r, rows)
        pl.semaphore_signal(barrier, inc=1, device_id={"row": peer}, device_id_type=MESH)

    def z_copy(c, j, r):
        t = c * count + j
        peer = lax.rem(at_col + r, cols)
        used = pl.ds(0, pieces[j][1] * held)
        return pltpu.make_async_remote_copy(
            src_ref=sent.at[j, peer, used], dst_ref=came.at[t, at_col, used],
            send_sem=send_z.at[t, r], recv_sem=recv_z.at[t, r],
            device_id={"col": peer}, device_id_type=MESH)

    def y_copy(c, j, r):
        peer = lax.rem(at_row + r, rows)
        return pltpu.make_async_remote_copy(
            src_ref=passed.at[j % slots, peer],
            dst_ref=out_ref.at[at_row, c, :, pl.ds(j * CHUNK, CHUNK), :],
            send_sem=send_y.at[c, j, r], recv_sem=recv_y.at[c, j, r],
            device_id={"row": peer}, device_id_type=MESH)

    def y_own(c, j):
        return pltpu.make_async_copy(
            passed.at[j % slots, at_row],
            out_ref.at[at_row, c, :, pl.ds(j * CHUNK, CHUNK), :], send_y.at[c, j, 0])

    def y_left(c, j):
        y_own(c, j).wait()
        for r in range(1, rows):
            y_copy(c, j, r).wait_send()

    def z_make(c, j):
        start, size = pieces[j]
        t = c * count + j
        if j == 0:
            load(c).wait()

        @pl.loop(0, size // group)
        def _(g):
            slabs = [modes[c, start + g * group + i] for i in range(group)]
            data = slabs[0] if group == 1 else jnp.concatenate(slabs, 0)
            value = jnp.dot(data, table_z[...], preferred_element_type=jnp.float32)
            value = value.astype(jnp.bfloat16)
            if value.shape[0] < block:
                spare = jnp.zeros((block - value.shape[0], value.shape[1]), jnp.bfloat16)
                value = jnp.concatenate([value, spare], 0)
            at = pl.ds(pl.multiple_of(g * block, 16), block)
            for b in range(cols):
                sent[j, b, at, :] = value[:, b * width : (b + 1) * width]
            came[t, at_col, at, :] = sent[j, at_col, at, :]

    def z_start(c, j):
        for i in reversed(range(cols - 1)):
            low, high = cols - 1 - i, i
            low = jnp.where(low <= at_col, low - 1, low)
            high = jnp.where(high >= at_col, high + 1, high)
            peer = jnp.where(at_col < cols // 2, low, high)
            z_copy(c, j, lax.rem(peer - at_col + cols, cols)).start()

    def ahead(c, j):
        return (c, j) if j < count else ahead(c + 1, j - count)

    total[...] = jnp.zeros_like(total)
    for u in range(min(WINDOW, 3 * count)):
        c, j = ahead(0, u)
        z_make(c, j)
        if u == 0:
            pl.semaphore_wait(barrier, cols + rows - 2)
        z_start(c, j)
    y_tables(table_y, held, ky)
    x_tables(table_x, rows, kx)
    phases(wave_ref, polar_ref, azimuth_ref, phase_ref, weight_ref, z_ref, y_ref, at_col, at_row)

    @pl.loop(0, 3)
    def _(c):
        for j, (start, size) in enumerate(pieces):
            t = c * count + j
            c_next, j_next = ahead(c, j + WINDOW)
            later = j + WINDOW >= count

            def make():
                if later:
                    for r in range(1, cols):
                        z_copy(c_next - 1, j_next, r).wait_send()
                else:
                    @pl.when(c > 0)
                    def _():
                        for r in range(1, cols):
                            z_copy(c - 1, j_next, r).wait_send()
                z_make(c_next, j_next)

            if later:
                pl.when(c_next < 3)(make)
            else:
                make()
            for r in range(1, cols):
                z_copy(c, j, r).wait_recv()
            if later:
                pl.when(c_next < 3)(functools.partial(z_start, c_next, j_next))
            else:
                z_start(c_next, j_next)

            @pl.loop(0, size // group)
            def _(g):
                at = pl.ds(pl.multiple_of(g * block, 16), block)
                blocks = [came[t, s, at, :] for s in range(cols)]
                lines = []
                for i in range(group):
                    parts = [part[i * held : (i + 1) * held] for part in blocks]
                    lines.append(jnp.concatenate(parts, 0))
                for i in range(0, group, pair):
                    line = lines[i] if pair == 1 else jnp.concatenate(lines[i : i + pair], 1)
                    ready[g * (group // pair) + i // pair] = line

            if j >= slots:
                y_left(c, j - slots)
            elif count - slots + j >= 0:
                @pl.when(c > 0)
                def _():
                    y_left(c - 1, count - slots + j)

            @pl.loop(0, rows)
            def _(q):
                step = jnp.where(lax.rem(at_row, 2) == 0, q, rows - q)
                r = lax.rem(step + rows // 2, rows)
                peer = lax.rem(at_row + r, rows)
                for a in range(0, size, pair):
                    product = jnp.dot(
                        table_y[peer], ready[a // pair], preferred_element_type=jnp.float32
                    )
                    for g in range(pair):
                        by_cos = product[:y_local, g * width : (g + 1) * width]
                        by_sin = product[y_local:, g * width : (g + 1) * width]
                        swap = jnp.concatenate([-by_sin[:, half:], by_sin[:, :half]], 1)
                        total[:, a + g, :] = by_cos + swap
                if size < CHUNK:
                    total[:, size:, :] = jnp.zeros((y_local, CHUNK - size, width), jnp.float32)
                passed[j % slots, peer] = total[...].astype(jnp.bfloat16)

                @pl.when(r == 0)
                def _():
                    y_own(c, j).start()

                @pl.when(r != 0)
                def _():
                    y_copy(c, j, r).start()

            if j == middle or j == count - 1:
                pl.when(c == 2)(functools.partial(x_early, j))

    for j in range(count):
        for r in range(1, rows):
            y_copy(2, j, r).wait_recv()

    for j in range(count):
        for r in range(1, cols):
            z_copy(2, j, r).wait_send()
    for j in range(max(count - slots, 0), count):
        y_left(2, j)


def gather(rows, cols, freqs, by_cos, by_sin, y_ref, out_ref, mine, wide, tall, sums,
           send_c, recv_c, send_r, recv_r):
    at_col, at_row = lax.axis_index("col"), lax.axis_index("row")
    barrier = pltpu.get_barrier_semaphore()
    for r in range(1, cols):
        peer = lax.rem(at_col + r, cols)
        pl.semaphore_signal(barrier, inc=1, device_id={"col": peer}, device_id_type=MESH)
    for r in range(1, rows):
        peer = lax.rem(at_row + r, rows)
        pl.semaphore_signal(barrier, inc=1, device_id={"row": peer}, device_id_type=MESH)

    def swapped(value):
        half = value.shape[1] // 2
        return jnp.concatenate([value[:, half:], -value[:, :half]], 1)

    both = by_cos[...] + swapped(by_sin[...])
    both = both * y_ref[0] + swapped(both) * y_ref[1]
    mine[...] = jnp.broadcast_to(jnp.sum(both, 0, keepdims=True), mine.shape)
    pl.semaphore_wait(barrier, cols + rows - 2)

    def col_copy(r):
        return pltpu.make_async_remote_copy(
            src_ref=mine, dst_ref=wide.at[r], send_sem=send_c.at[r], recv_sem=recv_c.at[r],
            device_id={"col": lax.rem(at_col + r, cols)}, device_id_type=MESH)

    def row_copy(r):
        return pltpu.make_async_remote_copy(
            src_ref=sums, dst_ref=tall.at[r], send_sem=send_r.at[r], recv_sem=recv_r.at[r],
            device_id={"row": lax.rem(at_row + r, rows)}, device_id_type=MESH)

    for r in range(1, cols):
        col_copy(r).start()
    result = mine[...]
    for r in range(1, cols):
        col_copy(r).wait_recv()
        result = result + wide[r]
    sums[...] = result
    for r in range(1, rows):
        row_copy(r).start()
    for r in range(1, rows):
        row_copy(r).wait_recv()
        result = result + tall[r]
    count = result.shape[1]
    dirs = count // (2 * freqs)
    lane = lax.broadcasted_iota(jnp.int32, result.shape, 1)
    part = lax.broadcasted_iota(jnp.int32, result.shape, 0)
    result = jnp.where((lane >= count // 2) == (part == 1), result, 0.0)
    shape = (count // 2, freqs)
    place = lax.broadcasted_iota(jnp.int32, shape, 0)
    freq = lax.broadcasted_iota(jnp.int32, shape, 1)
    for own in range(out_ref.shape[0]):
        direction = at_col * out_ref.shape[0] + own
        pick = jnp.where(place == freq * dirs + direction, 1.0, 0.0)
        pick = jnp.concatenate([pick, pick], 0)
        out_ref[own] = jnp.dot(
            result, pick, precision=lax.Precision.HIGHEST, preferred_element_type=jnp.float32
        )[:2]
    for r in range(1, cols):
        col_copy(r).wait_send()
    for r in range(1, rows):
        row_copy(r).wait_send()


def along_x(arrived_ref, early_ref, early_cos, early_sin, table_ref, phase_ref, weight_ref, z_ref,
            velocity_ref, by_cos_ref, by_sin_ref, real_scr, imag_scr):
    ys, width = arrived_ref.shape[2], arrived_ref.shape[4]
    half = width // 2
    for y in range(ys):
        data = arrived_ref[:, 0, y].reshape(-1, width).T
        real_scr[y * half : (y + 1) * half, :] = data[:half]
        imag_scr[y * half : (y + 1) * half, :] = data[half:]
    f2 = x_field(real_scr[...], imag_scr[...], table_ref)
    velocity_ref[2] = f2.astype(jnp.bfloat16).reshape(velocity_ref.shape[1:])
    velocity_ref[0] = early_ref[0]
    velocity_ref[1] = early_ref[1]
    f0 = early_ref[0].reshape(ys * half, -1).astype(jnp.float32)
    f1 = early_ref[1].reshape(ys * half, -1).astype(jnp.float32)
    by_cos, by_sin = x_lines(
        [f2 * f2, f0 * f2, f1 * f2], 3, phase_ref, weight_ref, z_ref, ys
    )
    by_cos_ref[...] = early_cos[...] + by_cos
    by_sin_ref[...] = early_sin[...] + by_sin


def body(rows, cols, velocity_modes, wavenumbers, polar, azimuth):
    kx_local, ky_local, modes = velocity_modes.shape[1:]
    modes = modes // 2
    points = velocity_points(modes)
    y_local, z_local = points // rows, points // cols
    width = 2 * z_local
    kx_pad = padded(kx_local)

    group, held = grouping(kx_local, ky_local)
    pair = 2 if group % 2 == 0 and width % 128 == 0 else 1
    count = len(pieces_of(kx_local))
    dirs, freqs = polar.shape[0], wavenumbers.shape[0]
    width_j = 2 * dirs * freqs
    depth = lanes(rows * kx_pad)
    table_z = z_table(modes, points, cols)
    arrived, early, early_cos, early_sin, table_x, phase, weights, near_z, near_y = pl.pallas_call(
        functools.partial(exchange, rows, cols),
        in_specs=[
            pl.BlockSpec(memory_space=pl.ANY),
            pl.BlockSpec(memory_space=pltpu.VMEM),
            *[pl.BlockSpec(memory_space=pltpu.SMEM)] * 3,
        ],
        out_specs=[
            pl.BlockSpec(memory_space=pl.ANY),
            pl.BlockSpec(memory_space=pl.ANY),
            *[pl.BlockSpec(memory_space=pltpu.VMEM)] * 7,
        ],
        out_shape=[
            jax.ShapeDtypeStruct((rows, 3, y_local, kx_pad, width), jnp.bfloat16),
            jax.ShapeDtypeStruct((2, y_local, z_local, points), jnp.bfloat16),
            jax.ShapeDtypeStruct((y_local, width_j), jnp.float32),
            jax.ShapeDtypeStruct((y_local, width_j), jnp.float32),
            jax.ShapeDtypeStruct((2 * depth, points), jnp.bfloat16),
            jax.ShapeDtypeStruct((points, width_j), jnp.bfloat16),
            jax.ShapeDtypeStruct((8, width_j), jnp.float32),
            jax.ShapeDtypeStruct((2, z_local, width_j), jnp.float32),
            jax.ShapeDtypeStruct((2, y_local, width_j), jnp.float32),
        ],
        scratch_shapes=[
            pltpu.VMEM((2, 2, rows, 8, kx_pad, width), jnp.bfloat16),
            pltpu.VMEM((2, 8 * z_local, rows * kx_pad), jnp.bfloat16),
            pltpu.VMEM((2, 8 * z_local, rows * kx_pad), jnp.bfloat16),
            pltpu.VMEM((2, 2, 8, z_local, points), jnp.bfloat16),
            pltpu.SemaphoreType.DMA((2, 2)),
            pltpu.SemaphoreType.DMA((2, 2)),
            pltpu.VMEM((rows, 2 * y_local, cols * held), jnp.bfloat16),
            pltpu.VMEM(velocity_modes.shape, jnp.bfloat16),
            pltpu.VMEM((count, cols, CHUNK * held, width), jnp.bfloat16),
            pltpu.VMEM((3 * count, cols, CHUNK * held, width), jnp.bfloat16),
            pltpu.VMEM((CHUNK // pair, cols * held, pair * width), jnp.bfloat16),
            pltpu.VMEM((y_local, CHUNK, width), jnp.float32),
            pltpu.VMEM((min(SLOTS, count), rows, y_local, CHUNK, width), jnp.bfloat16),
            pltpu.SemaphoreType.DMA((3,)),
            pltpu.SemaphoreType.DMA((3 * count, cols)),
            pltpu.SemaphoreType.DMA((3 * count, cols)),
            pltpu.SemaphoreType.DMA((3, count, rows)),
            pltpu.SemaphoreType.DMA((3, count, rows)),
        ],
        compiler_params=pltpu.CompilerParams(
            vmem_limit_bytes=VMEM_LIMIT, collective_id=0, has_side_effects=True
        ),
        cost_estimate=estimate(3 * 2 * points, cols * ky_local, 2 * kx_local * width),
        name="exchange",
    )(velocity_modes, table_z, wavenumbers, polar, azimuth)

    ys = 16
    whole = lambda i: (0, 0)
    velocity, by_cos, by_sin = pl.pallas_call(
        along_x,
        grid=(y_local // ys,),
        in_specs=[
            pl.BlockSpec((rows, 1, ys, kx_pad, width), lambda i: (0, 2, i, 0, 0)),
            pl.BlockSpec((2, ys, z_local, points), lambda i: (0, i, 0, 0)),
            pl.BlockSpec((ys, width_j), lambda i: (i, 0)),
            pl.BlockSpec((ys, width_j), lambda i: (i, 0)),
            pl.BlockSpec((2 * depth, points), whole),
            pl.BlockSpec((points, width_j), whole),
            pl.BlockSpec((8, width_j), whole),
            pl.BlockSpec((2, z_local, width_j), lambda i: (0, 0, 0)),
        ],
        out_specs=[
            pl.BlockSpec((3, ys, z_local, points), lambda i: (0, i, 0, 0)),
            pl.BlockSpec((ys, width_j), lambda i: (i, 0)),
            pl.BlockSpec((ys, width_j), lambda i: (i, 0)),
        ],
        out_shape=[
            jax.ShapeDtypeStruct((3, y_local, z_local, points), jnp.bfloat16),
            jax.ShapeDtypeStruct((y_local, width_j), jnp.float32),
            jax.ShapeDtypeStruct((y_local, width_j), jnp.float32),
        ],
        scratch_shapes=[
            pltpu.VMEM((ys * z_local, rows * kx_pad), jnp.bfloat16),
            pltpu.VMEM((ys * z_local, rows * kx_pad), jnp.bfloat16),
        ],
        compiler_params=pltpu.CompilerParams(vmem_limit_bytes=VMEM_LIMIT),
        name="along_x",
    )(
        arrived,
        early,
        early_cos,
        early_sin,
        table_x,
        phase,
        weights,
        near_z,
    )
    peers = lambda n: pltpu.SemaphoreType.DMA((n,))
    tile = (8, width_j)
    far_field = pl.pallas_call(
        functools.partial(gather, rows, cols, freqs),
        in_specs=[pl.BlockSpec(memory_space=pltpu.VMEM)] * 3,
        out_specs=pl.BlockSpec(memory_space=pltpu.VMEM),
        out_shape=jax.ShapeDtypeStruct((dirs // cols, 2, freqs), jnp.float32),
        scratch_shapes=[
            pltpu.VMEM(tile, jnp.float32),
            pltpu.VMEM((cols, *tile), jnp.float32),
            pltpu.VMEM((rows, *tile), jnp.float32),
            pltpu.VMEM(tile, jnp.float32),
            peers(cols), peers(cols), peers(rows), peers(rows),
        ],
        compiler_params=pltpu.CompilerParams(collective_id=1, has_side_effects=True),
        name="gather",
    )(by_cos, by_sin, near_y)
    return (velocity, far_field)


def velocity_points(modes):
    return 1 << (modes - 1).bit_length()


def solution(mesh):
    return jax.shard_map(
        functools.partial(body, mesh.shape["row"], mesh.shape["col"]),
        mesh=mesh,
        in_specs=(P(None, "row", "col", None), P(), P(), P()),
        out_specs=(P(None, "row", "col", None), P("col", None, None)),
        check_vma=False,
    )
```

```python
import functools
import math

import jax
import jax.numpy as jnp
import numpy as np
from jax import lax
from jax.experimental import pallas as pl
from jax.experimental.pallas import tpu as pltpu
from jax.sharding import PartitionSpec as P

VMEM_LIMIT = 60 * 1024 * 1024


def padded(count):
    return -(-count // 16) * 16


def lanes(count):
    return -(-count // 128) * 128


def circle(waves, cells, points):
    angle = np.mod(np.outer(waves, cells), points).astype(np.float64) * (2.0 * math.pi / points)
    return np.cos(angle).astype(np.float32), np.sin(angle).astype(np.float32)


def z_table(modes, points, blocks):
    cosine, sine = circle(np.arange(modes) - modes // 2, np.arange(points), points)
    cosine, sine = (part.reshape(modes, blocks, 1, -1) for part in (cosine, sine))
    table = np.concatenate(
        [np.concatenate([cosine, sine], 2), np.concatenate([-sine, cosine], 2)], 0
    )
    return jnp.asarray(table.reshape(2 * modes, 2 * points).astype(jnp.bfloat16))


def estimate(rows, depth, columns):
    return pl.CostEstimate(
        flops=2 * rows * depth * columns,
        bytes_accessed=2 * (rows * depth + depth * columns + rows * columns),
        transcendentals=0,
    )


MESH = pl.DeviceIdType.MESH
CHUNK = 8
SLOTS = 3
WINDOW = 2


def grouping(kx, ky):
    if kx % 4 == 0 and ky % 4 == 0:
        return 4, ky
    return 1, padded(ky)


def pieces_of(kx):
    first = kx % CHUNK or CHUNK
    starts = [0, *range(first, kx, CHUNK)]
    return [(start, CHUNK if start else first) for start in starts]


def spread(ref, inner, shape):
    lane = lax.broadcasted_iota(jnp.int32, shape, 1)
    count = ref.shape[0]
    total = jnp.zeros(shape, jnp.float32)
    for start in range(0, shape[1], inner):
        here = jnp.logical_and(lane >= start, lane < start + inner)
        total = jnp.where(here, ref[(start // inner) % count], total)
    return total


def turn(waves, cells, points):
    product = jnp.bitwise_and(waves * cells, points - 1)
    return product.astype(jnp.float32) * (2.0 * math.pi / points)


def y_tables(table_y, held, ky):
    blocks, double, depth = table_y.shape
    cells = double // 2
    points = blocks * cells
    modes = depth // held * ky
    tile = min(cells, 64)

    @pl.loop(0, points // tile)
    def _(i):
        shape = (tile, depth)
        lane = lax.broadcasted_iota(jnp.int32, shape, 1)
        source = jnp.floor((lane.astype(jnp.float32) + 0.5) / held).astype(jnp.int32)
        slot = lane - source * held
        cell = lax.broadcasted_iota(jnp.int32, shape, 0) + i * tile
        angle = turn(source * ky + slot - modes // 2, cell, points)
        block = i // (cells // tile)
        at = pl.multiple_of(lax.rem(i, cells // tile) * tile, tile)
        for base, part in ((0, jnp.cos(angle)), (cells, jnp.sin(angle))):
            part = jnp.where(slot < ky, part, 0.0).astype(jnp.bfloat16)
            table_y[block, pl.ds(base + at, tile), :] = part


def x_tables(table_x, rows, kx):
    depth, points = table_x.shape[0] // 2, table_x.shape[1]
    held = padded(kx)
    first = pieces_of(kx)[0][1]
    table_x[...] = jnp.zeros_like(table_x)

    @pl.loop(0, rows)
    def _(source):
        shape = (held, points)
        slot = lax.broadcasted_iota(jnp.int32, shape, 0)
        local = jnp.where(slot < first, slot, slot - (CHUNK - first))
        keep = jnp.logical_and(
            jnp.logical_or(slot < first, slot >= CHUNK), local < kx
        )
        wave = source * kx + local
        angle = turn(wave, lax.broadcasted_iota(jnp.int32, shape, 1), points)
        factor = jnp.where(keep, jnp.where(wave == 0, 1.0, 2.0), 0.0)
        for base, part in ((0, jnp.cos(angle)), (depth, -jnp.sin(angle))):
            part = factor * part.astype(jnp.bfloat16).astype(jnp.float32)
            at = pl.ds(pl.multiple_of(base + source * held, 16), held)
            table_x[at, :] = part.astype(jnp.bfloat16)


def phases(wave_ref, polar_ref, azimuth_ref, phase_ref, weight_ref, z_ref, y_ref, at_col, at_row):
    points, count = phase_ref.shape
    dirs = polar_ref.shape[0]
    row = (1, count)
    wave = spread(wave_ref, dirs, row)
    polar, azimuth = spread(polar_ref, 1, row), spread(azimuth_ref, 1, row)
    one = jnp.sin(polar) * jnp.cos(azimuth)
    two = jnp.sin(polar) * jnp.sin(azimuth)
    three = jnp.cos(polar)
    unit = 2.0 * math.pi / points

    def angle(axis, first, shape):
        at = lax.broadcasted_iota(jnp.int32, shape, 0) + first
        return wave * (axis * (at.astype(jnp.float32) * unit))

    square = [one * one, two * two, three * three]
    trace = (square[0] + square[1] + square[2]) / 3.0
    weights = [
        square[0] - trace,
        square[1] - trace,
        2.0 * one * two,
        square[2] - trace,
        2.0 * one * three,
        2.0 * two * three,
    ]
    for index, weight in enumerate(weights):
        weight_ref[index : index + 1, :] = weight
    weight_ref[6:8, :] = jnp.zeros((2, count), jnp.float32)
    tile = min(points, 64)

    @pl.loop(0, points // tile)
    def _(i):
        shape = (tile, count)
        at = angle(one, i * tile, shape)
        real = lax.broadcasted_iota(jnp.int32, shape, 1) < count // 2
        phase = jnp.where(real, jnp.cos(at), -jnp.sin(at))
        phase_ref[pl.ds(pl.multiple_of(i * tile, tile), tile), :] = phase.astype(jnp.bfloat16)

    for ref, axis, where, scale in (
        (z_ref, three, at_col, 1.0),
        (y_ref, two, at_row, wave * wave / points**1.5),
    ):
        held = ref.shape[1]
        at = angle(axis, where * held, (held, count))
        ref[0] = jnp.cos(at) * scale
        ref[1] = jnp.sin(at) * scale


def x_field(real, imag, table_ref):
    held, depth = real.shape[1], table_ref.shape[0] // 2
    field = jnp.dot(real, table_ref[0:held], preferred_element_type=jnp.float32)
    return field + jnp.dot(
        imag, table_ref[depth : depth + held], preferred_element_type=jnp.float32
    )


def x_lines(stress, first, phase_ref, weight_ref, z_ref, ys):
    mixed = None
    for index, part in enumerate(stress):
        line = jnp.dot(
            part.astype(jnp.bfloat16), phase_ref[...], preferred_element_type=jnp.float32
        )
        term = weight_ref[first + index : first + index + 1, :] * line
        mixed = term if mixed is None else mixed + term
    mixed = mixed.reshape(ys, -1, mixed.shape[1])
    return jnp.sum(mixed * z_ref[0][None], 1), jnp.sum(mixed * z_ref[1][None], 1)


def exchange(rows, cols, modes_ref, table_z, wave_ref, polar_ref, azimuth_ref,
             out_ref, early_ref, early_cos, early_sin, table_x, phase_ref, weight_ref, z_ref, y_ref,
             x_in, x_real, x_imag, x_out, in_x, out_x, table_y, modes, sent, came, ready, total, passed,
             in_sem, send_z, recv_z, send_y, recv_y):
    kx, ky = modes.shape[1], modes.shape[2]
    width = came.shape[3]
    half = width // 2
    y_local = out_ref.shape[2]
    at_col, at_row = lax.axis_index("col"), lax.axis_index("row")
    group, held = grouping(kx, ky)
    block = group * held
    pieces = pieces_of(kx)
    count = len(pieces)
    pair = ready.shape[2] // width
    slots = passed.shape[0]
    ys = x_in.shape[3]
    y_blocks = y_local // ys

    def x_load(b, e):
        slot = lax.rem(b, 2)
        at = pl.ds(pl.multiple_of(b * ys, ys), ys)
        return pltpu.make_async_copy(
            out_ref.at[:, e, at], x_in.at[slot, e], in_x.at[slot, e])

    def x_store(b, e):
        slot = lax.rem(b, 2)
        at = pl.ds(pl.multiple_of(b * ys, ys), ys)
        return pltpu.make_async_copy(
            x_out.at[slot, e], early_ref.at[e, at], out_x.at[slot, e])

    def x_run(low, high):
        for e in range(2):
            x_load(low, e).start()

        @pl.loop(low, high)
        def _(b):
            slot = lax.rem(b, 2)

            @pl.when(b + 1 < high)
            def _():
                for e in range(2):
                    x_load(b + 1, e).start()

            for e in range(2):
                x_load(b, e).wait()

            @pl.when(b >= low + 2)
            def _():
                for e in range(2):
                    x_store(b - 2, e).wait()

            fields = []
            for e in range(2):
                for y in range(ys):
                    data = x_in[slot, e, :, y].reshape(-1, width).T
                    x_real[e, y * half : (y + 1) * half, :] = data[:half]
                    x_imag[e, y * half : (y + 1) * half, :] = data[half:]
                field = x_field(x_real[e], x_imag[e], table_x)
                x_out[slot, e] = field.astype(jnp.bfloat16).reshape(x_out.shape[2:])
                fields.append(field)
            for e in range(2):
                x_store(b, e).start()
            f0, f1 = fields
            at = pl.ds(pl.multiple_of(b * ys, ys), ys)
            early_cos[at, :], early_sin[at, :] = x_lines(
                [f0 * f0, f1 * f1, f0 * f1], 0, phase_ref, weight_ref, z_ref, ys
            )

        for b in range(max(low, high - 2), high):
            for e in range(2):
                x_store(b, e).wait()

    middle = count // 2
    if middle < slots - 1 or middle >= count - 1 or y_blocks % 2:
        middle = None
    share = y_blocks * 5 // 8 if middle is not None else 0

    def x_early(j):
        if j == (count - 1 if middle is None else middle):
            for c in range(2):
                for i in range(count):
                    for r in range(1, rows):
                        y_copy(c, i, r).wait_recv()
        if j == middle:
            x_run(0, share)
        if j == count - 1:
            x_run(share, y_blocks)

    def load(c):
        return pltpu.make_async_copy(modes_ref.at[c], modes.at[c], in_sem.at[c])

    for c in range(3):
        load(c).start()
    barrier = pltpu.get_barrier_semaphore()
    for r in range(1, cols):
        peer = lax.rem(at_col + r, cols)
        pl.semaphore_signal(barrier, inc=1, device_id={"col": peer}, device_id_type=MESH)
    for r in range(1, rows):
        peer = lax.rem(at_row + r, rows)
        pl.semaphore_signal(barrier, inc=1, device_id={"row": peer}, device_id_type=MESH)

    def z_copy(c, j, r):
        t = c * count + j
        peer = lax.rem(at_col + r, cols)
        used = pl.ds(0, pieces[j][1] * held)
        return pltpu.make_async_remote_copy(
            src_ref=sent.at[j, peer, used], dst_ref=came.at[t, at_col, used],
            send_sem=send_z.at[t, r], recv_sem=recv_z.at[t, r],
            device_id={"col": peer}, device_id_type=MESH)

    def y_copy(c, j, r):
        peer = lax.rem(at_row + r, rows)
        return pltpu.make_async_remote_copy(
            src_ref=passed.at[j % slots, peer],
            dst_ref=out_ref.at[at_row, c, :, pl.ds(j * CHUNK, CHUNK), :],
            send_sem=send_y.at[c, j, r], recv_sem=recv_y.at[c, j, r],
            device_id={"row": peer}, device_id_type=MESH)

    def y_own(c, j):
        return pltpu.make_async_copy(
            passed.at[j % slots, at_row],
            out_ref.at[at_row, c, :, pl.ds(j * CHUNK, CHUNK), :], send_y.at[c, j, 0])

    def y_left(c, j):
        y_own(c, j).wait()
        for r in range(1, rows):
            y_copy(c, j, r).wait_send()

    def z_make(c, j):
        start, size = pieces[j]
        t = c * count + j
        if j == 0:
            load(c).wait()

        @pl.loop(0, size // group)
        def _(g):
            slabs = [modes[c, start + g * group + i] for i in range(group)]
            data = slabs[0] if group == 1 else jnp.concatenate(slabs, 0)
            value = jnp.dot(data, table_z[...], preferred_element_type=jnp.float32)
            value = value.astype(jnp.bfloat16)
            if value.shape[0] < block:
                spare = jnp.zeros((block - value.shape[0], value.shape[1]), jnp.bfloat16)
                value = jnp.concatenate([value, spare], 0)
            at = pl.ds(pl.multiple_of(g * block, 16), block)
            for b in range(cols):
                sent[j, b, at, :] = value[:, b * width : (b + 1) * width]
            came[t, at_col, at, :] = sent[j, at_col, at, :]

    def z_start(c, j):
        for i in reversed(range(cols - 1)):
            low, high = cols - 1 - i, i
            low = jnp.where(low <= at_col, low - 1, low)
            high = jnp.where(high >= at_col, high + 1, high)
            peer = jnp.where(at_col < cols // 2, low, high)
            z_copy(c, j, lax.rem(peer - at_col + cols, cols)).start()

    def ahead(c, j):
        return (c, j) if j < count else ahead(c + 1, j - count)

    total[...] = jnp.zeros_like(total)
    for u in range(min(WINDOW, 3 * count)):
        c, j = ahead(0, u)
        z_make(c, j)
        if u == 0:
            pl.semaphore_wait(barrier, cols + rows - 2)
        z_start(c, j)
    y_tables(table_y, held, ky)
    x_tables(table_x, rows, kx)
    phases(wave_ref, polar_ref, azimuth_ref, phase_ref, weight_ref, z_ref, y_ref, at_col, at_row)

    @pl.loop(0, 3)
    def _(c):
        for j, (start, size) in enumerate(pieces):
            t = c * count + j
            c_next, j_next = ahead(c, j + WINDOW)
            later = j + WINDOW >= count

            def make():
                if later:
                    for r in range(1, cols):
                        z_copy(c_next - 1, j_next, r).wait_send()
                else:
                    @pl.when(c > 0)
                    def _():
                        for r in range(1, cols):
                            z_copy(c - 1, j_next, r).wait_send()
                z_make(c_next, j_next)

            if later:
                pl.when(c_next < 3)(make)
            else:
                make()
            for r in range(1, cols):
                z_copy(c, j, r).wait_recv()
            if later:
                pl.when(c_next < 3)(functools.partial(z_start, c_next, j_next))
            else:
                z_start(c_next, j_next)

            @pl.loop(0, size // group)
            def _(g):
                at = pl.ds(pl.multiple_of(g * block, 16), block)
                blocks = [came[t, s, at, :] for s in range(cols)]
                lines = []
                for i in range(group):
                    parts = [part[i * held : (i + 1) * held] for part in blocks]
                    lines.append(jnp.concatenate(parts, 0))
                for i in range(0, group, pair):
                    line = lines[i] if pair == 1 else jnp.concatenate(lines[i : i + pair], 1)
                    ready[g * (group // pair) + i // pair] = line

            if j >= slots:
                y_left(c, j - slots)
            elif count - slots + j >= 0:
                @pl.when(c > 0)
                def _():
                    y_left(c - 1, count - slots + j)

            @pl.loop(0, rows)
            def _(q):
                step = jnp.where(lax.rem(at_row, 2) == 0, q, rows - q)
                r = lax.rem(step + rows // 2, rows)
                peer = lax.rem(at_row + r, rows)
                for a in range(0, size, pair):
                    product = jnp.dot(
                        table_y[peer], ready[a // pair], preferred_element_type=jnp.float32
                    )
                    for g in range(pair):
                        by_cos = product[:y_local, g * width : (g + 1) * width]
                        by_sin = product[y_local:, g * width : (g + 1) * width]
                        swap = jnp.concatenate([-by_sin[:, half:], by_sin[:, :half]], 1)
                        total[:, a + g, :] = by_cos + swap
                if size < CHUNK:
                    total[:, size:, :] = jnp.zeros((y_local, CHUNK - size, width), jnp.float32)
                passed[j % slots, peer] = total[...].astype(jnp.bfloat16)

                @pl.when(r == 0)
                def _():
                    y_own(c, j).start()

                @pl.when(r != 0)
                def _():
                    y_copy(c, j, r).start()

            if j == middle or j == count - 1:
                pl.when(c == 2)(functools.partial(x_early, j))

    for j in range(count):
        for r in range(1, rows):
            y_copy(2, j, r).wait_recv()

    for j in range(count):
        for r in range(1, cols):
            z_copy(2, j, r).wait_send()
    for j in range(max(count - slots, 0), count):
        y_left(2, j)


def gather(rows, cols, freqs, by_cos, by_sin, y_ref, out_ref, mine, wide, tall, sums,
           send_c, recv_c, send_r, recv_r):
    at_col, at_row = lax.axis_index("col"), lax.axis_index("row")
    barrier = pltpu.get_barrier_semaphore()
    for r in range(1, cols):
        peer = lax.rem(at_col + r, cols)
        pl.semaphore_signal(barrier, inc=1, device_id={"col": peer}, device_id_type=MESH)
    for r in range(1, rows):
        peer = lax.rem(at_row + r, rows)
        pl.semaphore_signal(barrier, inc=1, device_id={"row": peer}, device_id_type=MESH)

    def swapped(value):
        half = value.shape[1] // 2
        return jnp.concatenate([value[:, half:], -value[:, :half]], 1)

    both = by_cos[...] + swapped(by_sin[...])
    both = both * y_ref[0] + swapped(both) * y_ref[1]
    mine[...] = jnp.broadcast_to(jnp.sum(both, 0, keepdims=True), mine.shape)
    pl.semaphore_wait(barrier, cols + rows - 2)

    def col_copy(r):
        return pltpu.make_async_remote_copy(
            src_ref=mine, dst_ref=wide.at[r], send_sem=send_c.at[r], recv_sem=recv_c.at[r],
            device_id={"col": lax.rem(at_col + r, cols)}, device_id_type=MESH)

    def row_copy(r):
        return pltpu.make_async_remote_copy(
            src_ref=sums, dst_ref=tall.at[r], send_sem=send_r.at[r], recv_sem=recv_r.at[r],
            device_id={"row": lax.rem(at_row + r, rows)}, device_id_type=MESH)

    for r in range(1, cols):
        col_copy(r).start()
    result = mine[...]
    for r in range(1, cols):
        col_copy(r).wait_recv()
        result = result + wide[r]
    sums[...] = result
    for r in range(1, rows):
        row_copy(r).start()
    for r in range(1, rows):
        row_copy(r).wait_recv()
        result = result + tall[r]
    count = result.shape[1]
    dirs = count // (2 * freqs)
    lane = lax.broadcasted_iota(jnp.int32, result.shape, 1)
    part = lax.broadcasted_iota(jnp.int32, result.shape, 0)
    result = jnp.where((lane >= count // 2) == (part == 1), result, 0.0)
    shape = (count // 2, freqs)
    place = lax.broadcasted_iota(jnp.int32, shape, 0)
    freq = lax.broadcasted_iota(jnp.int32, shape, 1)
    for own in range(out_ref.shape[0]):
        direction = at_col * out_ref.shape[0] + own
        pick = jnp.where(place == freq * dirs + direction, 1.0, 0.0)
        pick = jnp.concatenate([pick, pick], 0)
        out_ref[own] = jnp.dot(
            result, pick, precision=lax.Precision.HIGHEST, preferred_element_type=jnp.float32
        )[:2]
    for r in range(1, cols):
        col_copy(r).wait_send()
    for r in range(1, rows):
        row_copy(r).wait_send()


def along_x(arrived_ref, early_ref, early_cos, early_sin, table_ref, phase_ref, weight_ref, z_ref,
            velocity_ref, by_cos_ref, by_sin_ref, real_scr, imag_scr):
    ys, width = arrived_ref.shape[2], arrived_ref.shape[4]
    half = width // 2
    for y in range(ys):
        data = arrived_ref[:, 0, y].reshape(-1, width).T
        real_scr[y * half : (y + 1) * half, :] = data[:half]
        imag_scr[y * half : (y + 1) * half, :] = data[half:]
    f2 = x_field(real_scr[...], imag_scr[...], table_ref)
    velocity_ref[2] = f2.astype(jnp.bfloat16).reshape(velocity_ref.shape[1:])
    velocity_ref[0] = early_ref[0]
    velocity_ref[1] = early_ref[1]
    f0 = early_ref[0].reshape(ys * half, -1).astype(jnp.float32)
    f1 = early_ref[1].reshape(ys * half, -1).astype(jnp.float32)
    by_cos, by_sin = x_lines(
        [f2 * f2, f0 * f2, f1 * f2], 3, phase_ref, weight_ref, z_ref, ys
    )
    by_cos_ref[...] = early_cos[...] + by_cos
    by_sin_ref[...] = early_sin[...] + by_sin


def body(rows, cols, velocity_modes, wavenumbers, polar, azimuth):
    kx_local, ky_local, modes = velocity_modes.shape[1:]
    modes = modes // 2
    points = velocity_points(modes)
    y_local, z_local = points // rows, points // cols
    width = 2 * z_local
    kx_pad = padded(kx_local)

    group, held = grouping(kx_local, ky_local)
    pair = 2 if group % 2 == 0 and width % 128 == 0 else 1
    count = len(pieces_of(kx_local))
    dirs, freqs = polar.shape[0], wavenumbers.shape[0]
    width_j = 2 * dirs * freqs
    depth = lanes(rows * kx_pad)
    table_z = z_table(modes, points, cols)
    arrived, early, early_cos, early_sin, table_x, phase, weights, near_z, near_y = pl.pallas_call(
        functools.partial(exchange, rows, cols),
        in_specs=[
            pl.BlockSpec(memory_space=pl.ANY),
            pl.BlockSpec(memory_space=pltpu.VMEM),
            *[pl.BlockSpec(memory_space=pltpu.SMEM)] * 3,
        ],
        out_specs=[
            pl.BlockSpec(memory_space=pl.ANY),
            pl.BlockSpec(memory_space=pl.ANY),
            *[pl.BlockSpec(memory_space=pltpu.VMEM)] * 7,
        ],
        out_shape=[
            jax.ShapeDtypeStruct((rows, 3, y_local, kx_pad, width), jnp.bfloat16),
            jax.ShapeDtypeStruct((2, y_local, z_local, points), jnp.bfloat16),
            jax.ShapeDtypeStruct((y_local, width_j), jnp.float32),
            jax.ShapeDtypeStruct((y_local, width_j), jnp.float32),
            jax.ShapeDtypeStruct((2 * depth, points), jnp.bfloat16),
            jax.ShapeDtypeStruct((points, width_j), jnp.bfloat16),
            jax.ShapeDtypeStruct((8, width_j), jnp.float32),
            jax.ShapeDtypeStruct((2, z_local, width_j), jnp.float32),
            jax.ShapeDtypeStruct((2, y_local, width_j), jnp.float32),
        ],
        scratch_shapes=[
            pltpu.VMEM((2, 2, rows, 8, kx_pad, width), jnp.bfloat16),
            pltpu.VMEM((2, 8 * z_local, rows * kx_pad), jnp.bfloat16),
            pltpu.VMEM((2, 8 * z_local, rows * kx_pad), jnp.bfloat16),
            pltpu.VMEM((2, 2, 8, z_local, points), jnp.bfloat16),
            pltpu.SemaphoreType.DMA((2, 2)),
            pltpu.SemaphoreType.DMA((2, 2)),
            pltpu.VMEM((rows, 2 * y_local, cols * held), jnp.bfloat16),
            pltpu.VMEM(velocity_modes.shape, jnp.bfloat16),
            pltpu.VMEM((count, cols, CHUNK * held, width), jnp.bfloat16),
            pltpu.VMEM((3 * count, cols, CHUNK * held, width), jnp.bfloat16),
            pltpu.VMEM((CHUNK // pair, cols * held, pair * width), jnp.bfloat16),
            pltpu.VMEM((y_local, CHUNK, width), jnp.float32),
            pltpu.VMEM((min(SLOTS, count), rows, y_local, CHUNK, width), jnp.bfloat16),
            pltpu.SemaphoreType.DMA((3,)),
            pltpu.SemaphoreType.DMA((3 * count, cols)),
            pltpu.SemaphoreType.DMA((3 * count, cols)),
            pltpu.SemaphoreType.DMA((3, count, rows)),
            pltpu.SemaphoreType.DMA((3, count, rows)),
        ],
        compiler_params=pltpu.CompilerParams(
            vmem_limit_bytes=VMEM_LIMIT, collective_id=0, has_side_effects=True
        ),
        cost_estimate=estimate(3 * 2 * points, cols * ky_local, 2 * kx_local * width),
        name="exchange",
    )(velocity_modes, table_z, wavenumbers, polar, azimuth)

    ys = 16
    whole = lambda i: (0, 0)
    velocity, by_cos, by_sin = pl.pallas_call(
        along_x,
        grid=(y_local // ys,),
        in_specs=[
            pl.BlockSpec((rows, 1, ys, kx_pad, width), lambda i: (0, 2, i, 0, 0)),
            pl.BlockSpec((2, ys, z_local, points), lambda i: (0, i, 0, 0)),
            pl.BlockSpec((ys, width_j), lambda i: (i, 0)),
            pl.BlockSpec((ys, width_j), lambda i: (i, 0)),
            pl.BlockSpec((2 * depth, points), whole),
            pl.BlockSpec((points, width_j), whole),
            pl.BlockSpec((8, width_j), whole),
            pl.BlockSpec((2, z_local, width_j), lambda i: (0, 0, 0)),
        ],
        out_specs=[
            pl.BlockSpec((3, ys, z_local, points), lambda i: (0, i, 0, 0)),
            pl.BlockSpec((ys, width_j), lambda i: (i, 0)),
            pl.BlockSpec((ys, width_j), lambda i: (i, 0)),
        ],
        out_shape=[
            jax.ShapeDtypeStruct((3, y_local, z_local, points), jnp.bfloat16),
            jax.ShapeDtypeStruct((y_local, width_j), jnp.float32),
            jax.ShapeDtypeStruct((y_local, width_j), jnp.float32),
        ],
        scratch_shapes=[
            pltpu.VMEM((ys * z_local, rows * kx_pad), jnp.bfloat16),
            pltpu.VMEM((ys * z_local, rows * kx_pad), jnp.bfloat16),
        ],
        compiler_params=pltpu.CompilerParams(vmem_limit_bytes=VMEM_LIMIT),
        name="along_x",
    )(
        arrived,
        early,
        early_cos,
        early_sin,
        table_x,
        phase,
        weights,
        near_z,
    )
    peers = lambda n: pltpu.SemaphoreType.DMA((n,))
    tile = (8, width_j)
    far_field = pl.pallas_call(
        functools.partial(gather, rows, cols, freqs),
        in_specs=[pl.BlockSpec(memory_space=pltpu.VMEM)] * 3,
        out_specs=pl.BlockSpec(memory_space=pltpu.VMEM),
        out_shape=jax.ShapeDtypeStruct((dirs // cols, 2, freqs), jnp.float32),
        scratch_shapes=[
            pltpu.VMEM(tile, jnp.float32),
            pltpu.VMEM((cols, *tile), jnp.float32),
            pltpu.VMEM((rows, *tile), jnp.float32),
            pltpu.VMEM(tile, jnp.float32),
            peers(cols), peers(cols), peers(rows), peers(rows),
        ],
        compiler_params=pltpu.CompilerParams(collective_id=1, has_side_effects=True),
        name="gather",
    )(by_cos, by_sin, near_y)
    return (velocity, far_field)


def velocity_points(modes):
    return 1 << (modes - 1).bit_length()


def solution(mesh):
    return jax.shard_map(
        functools.partial(body, mesh.shape["row"], mesh.shape["col"]),
        mesh=mesh,
        in_specs=(P(None, "row", "col", None), P(), P(), P()),
        out_specs=(P(None, "row", "col", None), P("col", None, None)),
        check_vma=False,
    )
```
